256 devices in a mesh: tm: 64 (over x, z, core), hid: 4 (over y).
Axes of the slice: x: 4, y: 4, z: 8, core: 2. Of those that a mesh axis runs over, the one named last changes fastest.
Arguments:
- token_ids: int32 [32768], P('tm'), may hold values from 0 to 255
- input_table: float32 [256, 3, 2048], P(None, None, 'hid'), may hold values from -6 to 6
- recur_weight: bfloat16 [2048, 3, 2048], P(None, None, 'hid'), may hold values from -0.125 to 0.125
- z_bias: float32 [2048], P('hid'), may hold values from -1 to 9
- hn_bias: float32 [2048], P('hid'), may hold values from -4 to 4
- init_state: float32 [2048], P('hid'), may hold values from -0.9 to 0.9
- guess: float32 [32768, 2048], P('tm', 'hid'), may hold values from -3 to 3
Outputs:
- states: float32 [32768, 2048], P('tm', 'hid')
- residual_norm: float32 [2], replicated
The draws below stay inside these ranges and needn't reach their ends.
All inputs are finite; a program needn't handle non-finite values.
Results may differ from the reference program's by a relative error of at most 0.00063.
Values may be sent and summed in bfloat16 or wider, within the bound.
A program may use at most 128 MiB of HBM per device.

```python
import math
import jax
import jax.numpy as jnp
import numpy as np
from jax import lax

H = 2048
V = 256
TOK_DEV = 512
ITERS = 2
TOKENS = 32768


def draw_guess(key, part):
    ramp = jnp.arange(TOKENS, dtype=jnp.float32) / TOKENS
    scale = 0.3 * jnp.exp(jnp.log(3.0) * ramp)
    values = jax.random.truncated_normal(key, -2.5, 2.5, (TOKENS, H), jnp.float32)
    return values * scale[:, None]


def set_ends(array, stream_key, low, top_value):
    index_at = [jax.random.randint(jax.random.fold_in(stream_key, axis), (), 0, length) for axis, length in enumerate(array.shape)]
    widest = array.shape.index(max(array.shape))
    neighbour = index_at[:widest] + [(index_at[widest] + 1) % array.shape[widest]] + index_at[widest + 1:]
    return array.at[tuple(index_at)].set(low).at[tuple(neighbour)].set(top_value)


def block_levels(key, extent, shards, least, high):
    factor_of, own = 1.0, jax.random.fold_in(key, 6)
    for position, parts in shards:
        heights = jnp.exp(jax.random.uniform(jax.random.fold_in(own, position), (parts,), jnp.float32, least / len(shards), high / len(shards)))
        factor_of = factor_of * jnp.repeat(heights, extent[position] // parts).reshape([-1 if axis == position else 1 for axis in range(len(extent))])
    return factor_of


def cumulative_ranks(number_of, lean):
    portions = [(1 << 20) // math.isqrt(grade ** lean) + 1 for grade in range(1, number_of + 1)]
    width = 1 + sum(portions) // (1 << 30)
    return np.cumsum(np.array([max(1, weight // width) for weight in portions]))


def skewed_ids(rng, extent, count, skew):
    listing = cumulative_ranks(count, skew)
    lot = jax.random.randint(jax.random.fold_in(rng, 1), extent, 0, int(listing[count - 1]))
    grade = jnp.searchsorted(jnp.asarray(listing, jnp.int32), lot, side="right")
    return jax.random.permutation(jax.random.fold_in(rng, 2), count)[grade].astype(jnp.int32)


def scatter_about(stream_key, extent, scale, bound, pieces=(), held_as=jnp.bfloat16):
    gain = block_levels(stream_key, extent, pieces, -0.22, 0.18) if pieces else 1.0
    array = jax.random.normal(stream_key, extent, jnp.float32) * scale * gain
    return jnp.minimum(jnp.maximum(array, -bound), bound).astype(held_as)


def setup_inputs(seed: int = 0) -> dict:
    key_of = jax.random.split(jax.random.key(seed), 8)
    token_ids = set_ends(skewed_ids(key_of[0], (TOKENS,), V, 2), jax.random.fold_in(key_of[0], 3), 0, V - 1).astype(jnp.int32)
    input_table = scatter_about(key_of[1], (V, 3, H), 1.0, 6.0, ((2, 4),), jnp.float32)
    recur_weight = scatter_about(key_of[2], (H, 3, H), H ** -0.5, 0.125, ((2, 4),))
    z_bias = jnp.clip(-1.0 + 10.0 * jax.random.uniform(key_of[3], (H,), jnp.float32) ** block_levels(key_of[3], (H,), ((0, 4),), -0.2, 0.2), -1.0, 9.0)
    hn_bias = scatter_about(key_of[4], (H,), 1.0, 4.0, ((0, 4),), jnp.float32)
    init_state = jnp.clip(jax.random.uniform(key_of[5], (H,), jnp.float32, -0.9, 0.9) * block_levels(key_of[5], (H,), ((0, 4),), -0.4, 0.0), -0.9, 0.9)
    guess = draw_guess(jax.random.fold_in(key_of[7], 71), 0)
    return dict(token_ids=token_ids, input_table=input_table, recur_weight=recur_weight, z_bias=z_bias, hn_bias=hn_bias, init_state=init_state, guess=guess)


def cell(prev, inputs, products, z_bias, hn_bias, diag_z, diag_r, diag_n):
    zeta = jax.nn.sigmoid(inputs[:, 0] + products[:, 0] + z_bias)
    reset = jax.nn.sigmoid(inputs[:, 1] + products[:, 1])
    cand_pre = products[:, 2] + hn_bias
    cand = jnp.tanh(inputs[:, 2] + reset * cand_pre)
    value = (1.0 - zeta) * cand + zeta * prev
    slope = zeta + (prev - cand) * zeta * (1.0 - zeta) * diag_z
    slope = slope + (1.0 - zeta) * (1.0 - cand * cand) * (reset * diag_n + cand_pre * reset * (1.0 - reset) * diag_r)
    return (value, slope)

def reference(token_ids, input_table, recur_weight, z_bias, hn_bias, init_state, guess):
    weight_mat = recur_weight.reshape(H, 3 * H)
    diag_z = jnp.diagonal(recur_weight[:, 0, :]).astype(jnp.float32)
    diag_r = jnp.diagonal(recur_weight[:, 1, :]).astype(jnp.float32)
    diag_n = jnp.diagonal(recur_weight[:, 2, :]).astype(jnp.float32)
    blocks = TOKENS // TOK_DEV
    state = guess
    norms = []
    for step in range(ITERS):
        prev = jnp.concatenate([init_state[None], state[:-1]], 0)

        def evaluate(packed):
            ids, prev_block, state_block = packed
            inputs = input_table[ids]
            products = jnp.dot(prev_block.astype(jnp.bfloat16), weight_mat, preferred_element_type=jnp.float32)
            products = products.reshape(prev_block.shape[0], 3, H)
            value, slope = cell(prev_block, inputs, products, z_bias, hn_bias, diag_z, diag_r, diag_n)
            return (value - slope * prev_block, slope, jnp.sum((state_block - value) ** 2))
        offsets, slopes, squares = lax.map(evaluate, (token_ids.reshape(blocks, TOK_DEV), prev.reshape(blocks, TOK_DEV, H), state.reshape(blocks, TOK_DEV, H)))
        norms.append(jnp.sqrt(jnp.sum(squares) / (TOKENS * H)))

        def advance(carry, pair):
            carry = pair[0] * carry + pair[1]
            return (carry, carry)
        _, state = lax.scan(advance, init_state, (slopes.reshape(TOKENS, H), offsets.reshape(TOKENS, H)))
    return (state, jnp.stack(norms))
```

```python
import functools

import jax
import jax.numpy as jnp
from jax import lax
from jax.experimental import pallas as pl
from jax.experimental.pallas import tpu as pltpu
from jax.sharding import Mesh
from jax.sharding import PartitionSpec as P

ITERS = 2
SEGS = 8
PAIRS = 4
LANES = 128
ORDER = (1, 0, 2, 3)
TM = ("tm_0", "tm_1", "tm_2")
MESH = pl.DeviceIdType.MESH
F32 = jnp.float32
BF16 = jnp.bfloat16


def dot(a, b):
    return jnp.dot(a, b, preferred_element_type=F32)


def sigmoid(x):
    return 0.5 * jnp.tanh(0.5 * x) + 0.5


def lanes_to_rows(row):
    return jnp.concatenate([row[:, k : k + LANES] for k in range(0, row.shape[1], LANES)], 0)


def rows_to_lanes(block):
    return jnp.concatenate([block[k : k + 1] for k in range(block.shape[0])], 1)


def wait_bytes(ref, sem):
    pltpu.make_async_copy(ref, ref, sem).wait()


def kernel(
    dims,
    ids_ref,
    table_hbm,
    weight_hbm,
    zb_ref,
    hb_ref,
    init_ref,
    guess_hbm,
    out_hbm,
    res_ref,
    table,
    pieces,
    weight,
    hist,
    sent,
    onehot,
    inp,
    acc,
    pre_a,
    pre_b,
    diag,
    seg,
    edge,
    line_maps,
    x_maps,
    line_res,
    plane_res,
    in_sem,
    weight_sem,
    out_sem,
    edge_sem,
    send_sem,
    recv_sem,
    relay_sem,
    line_sem,
    x_sem,
    res_sem,
):
    nx, nz, nc, ny, rows, width, vocab = dims
    steps = rows // SEGS
    block = rows // PAIRS
    group = block // SEGS
    tiles = width // LANES
    members = nz * nc
    plane = nx * ny
    x, z, c, y = (lax.axis_index(a) for a in (*TM, "hid"))
    mine = z * nc + c
    tm = x * members + mine
    right, left, far = (lax.rem(y + d, ny) for d in (1, ny - 1, 2))
    count = nx * members * rows * ny * width

    def line_peer(k):
        peer = lax.rem(mine + k, members)
        return {"tm_1": peer // nc, "tm_2": lax.rem(peer, nc)}

    def plane_peer(k):
        return {"tm_0": lax.rem(x + k // ny, nx), "hid": lax.rem(y + lax.rem(k, ny), ny)}

    def tm_peer(index):
        return {
            "tm_0": index // members,
            "tm_1": lax.rem(index, members) // nc,
            "tm_2": lax.rem(index, nc),
        }

    total = nx * members
    after, before = (lax.rem(tm + d, total) for d in (1, total - 1))

    barrier = pltpu.get_barrier_semaphore()

    def greet(peer):
        pl.semaphore_signal(barrier, inc=1, device_id=peer, device_id_type=MESH)

    greet(tm_peer(after))
    greet(tm_peer(before))
    lax.fori_loop(1, plane, lambda k, _: greet(plane_peer(k)), None)
    lax.fori_loop(1, members, lambda k, _: greet(line_peer(k)), None)

    for s in range(SEGS):
        pltpu.make_async_copy(
            guess_hbm.at[pl.ds(s * steps, steps)], hist.at[pl.ds(1, steps), s], in_sem.at[s]
        ).start()
    for s in range(SEGS):
        pltpu.make_async_copy(
            guess_hbm.at[pl.ds(s * steps, steps)], hist.at[pl.ds(1, steps), s], in_sem.at[s]
        ).wait()
    table_copy = pltpu.make_async_copy(table_hbm, table, weight_sem.at[0])
    weight_copy = pltpu.make_async_copy(weight_hbm, weight, weight_sem.at[1])
    pl.semaphore_wait(barrier, plane + members)

    edge_copy = pltpu.make_async_remote_copy(
        src_ref=hist.at[steps],
        dst_ref=edge,
        send_sem=edge_sem.at[0],
        recv_sem=edge_sem.at[1],
        device_id=tm_peer(after),
        device_id_type=MESH,
    )
    edge_copy.start()

    def piece(it, slot, p):
        return sent.at[it, slot, pl.ds(p * block, block)]

    def half(it, slot, p, h):
        return sent.at[it, slot, pl.ds(p * block + h * (block // 2), block // 2)]

    def direct(it, p, side, slot):
        return pltpu.make_async_remote_copy(
            src_ref=piece(it, slot, p),
            dst_ref=piece(it, slot, p),
            send_sem=send_sem.at[it],
            recv_sem=recv_sem.at[it, side, p],
            device_id={"hid": (right, left)[side]},
            device_id_type=MESH,
        )

    def relay(it, p, side, slot):
        return pltpu.make_async_remote_copy(
            src_ref=half(it, slot, p, side),
            dst_ref=half(it, slot, p, side),
            send_sem=send_sem.at[it],
            recv_sem=relay_sem.at[it, side, p],
            device_id={"hid": (right, left)[side]},
            device_id_type=MESH,
        )

    def block_rows(p):
        return pl.ds(pl.multiple_of(p * block, block), block)

    def weight_rows(slot):
        return pl.ds(pl.multiple_of(slot * width, width), width)

    def send_block(it, p):
        prev = hist[pl.ds(p * group, group)].reshape(block, width)
        sent[it, y, block_rows(p)] = prev.astype(BF16)
        direct(it, p, 0, y).start()
        direct(it, p, 1, y).start()

    def near_products(it):
        def visit(i, _):
            p = jnp.where(i < 2, 1 - i, i)
            direct(it, p, 0, left).wait_recv()
            relay(it, p, 0, left).start()
            direct(it, p, 1, right).wait_recv()
            relay(it, p, 1, right).start()

            def gate(g, _):
                part = dot(sent[it, y, block_rows(p)], weight[g, weight_rows(y)])
                part += dot(sent[it, left, block_rows(p)], weight[g, weight_rows(left)])
                part += dot(sent[it, right, block_rows(p)], weight[g, weight_rows(right)])
                acc[g, block_rows(p)] = part

            lax.fori_loop(0, 3, gate, None)

        lax.fori_loop(0, PAIRS, visit, None)

    def far_products(it, p):
        relay(it, p, 0, far).wait_recv()
        relay(it, p, 1, far).wait_recv()

        def gate(g, _):
            acc[g, block_rows(p)] += dot(sent[it, far, block_rows(p)], weight[g, weight_rows(far)])

        lax.fori_loop(0, 3, gate, None)

    def cells(it, p, carry):
        def visit(k, carry):
            run_a, run_b, err = carry
            j = p * group + k
            at = pl.ds(pl.multiple_of(j * SEGS, SEGS), SEGS)
            prev, state = hist[j], hist[j + 1]
            zeta = sigmoid(acc[0, at] + inp[0, at])
            reset = sigmoid(acc[1, at] + inp[1, at])
            cand_pre = acc[2, at] + hb_ref[...]
            cand = jnp.tanh(inp[2, at] + reset * cand_pre)
            moved = zeta * (prev - cand)
            value = cand + moved
            slope = reset * (diag[2] + cand_pre * (1.0 - reset) * diag[1])
            slope = moved * diag[0] + (1.0 - cand * cand) * slope
            slope = zeta + (1.0 - zeta) * slope
            gap = state - value
            run_a = slope * run_a
            run_b = slope * run_b + (value - slope * prev)
            pre_a[j] = run_a
            pre_b[j] = run_b
            return run_a, run_b, err + gap * gap

        return lax.fori_loop(0, group, visit, carry, unroll=2)

    def sweep(it):
        near_products(it)
        carry = (
            jnp.ones((SEGS, width), F32),
            jnp.zeros((SEGS, width), F32),
            jnp.zeros((SEGS, width), F32),
        )
        far_products(it, ORDER[0])
        far_products(it, ORDER[1])
        carry = cells(it, 0, carry)
        carry = cells(it, 1, carry)
        far_products(it, 2)
        carry = cells(it, 2, carry)
        far_products(it, 3)
        return cells(it, 3, carry)

    def line_copy(it, k):
        return pltpu.make_async_remote_copy(
            src_ref=line_maps.at[it, mine],
            dst_ref=line_maps.at[it, mine],
            send_sem=line_sem.at[it, 0],
            recv_sem=line_sem.at[it, 1],
            device_id=line_peer(k),
            device_id_type=MESH,
        )

    def x_copy(it, k):
        return pltpu.make_async_remote_copy(
            src_ref=x_maps.at[it, x],
            dst_ref=x_maps.at[it, x],
            send_sem=x_sem.at[it, 0],
            recv_sem=x_sem.at[it, 1],
            device_id={"tm_0": lax.rem(x + k, nx)},
            device_id_type=MESH,
        )

    def res_copy(k):
        return pltpu.make_async_remote_copy(
            src_ref=line_res.at[mine],
            dst_ref=line_res.at[mine],
            send_sem=res_sem.at[0],
            recv_sem=res_sem.at[1],
            device_id=line_peer(k),
            device_id_type=MESH,
        )

    def plane_copy(k):
        return pltpu.make_async_remote_copy(
            src_ref=plane_res.at[x * ny + y],
            dst_ref=plane_res.at[x * ny + y],
            send_sem=res_sem.at[2],
            recv_sem=res_sem.at[3],
            device_id=plane_peer(k),
            device_id_type=MESH,
        )

    def start(copy, k):
        copy(k).start()

    def entering(it, run_a, run_b, sums):
        map_a, map_b = jnp.ones((1, width), F32), jnp.zeros((1, width), F32)
        for s in range(SEGS):
            seg[0, s : s + 1] = map_a
            seg[1, s : s + 1] = map_b
            map_b = run_a[s : s + 1] * map_b + run_b[s : s + 1]
            map_a = run_a[s : s + 1] * map_a
        line_maps[it, mine] = jnp.concatenate([lanes_to_rows(map_a), lanes_to_rows(map_b)], 0)
        lax.fori_loop(1, members, lambda k, _: start(functools.partial(line_copy, it), k), None)
        if sums is not None:
            line_res[mine] = jnp.concatenate([jnp.sum(e, 0, keepdims=True) for e in sums], 0)
            lax.fori_loop(1, members, lambda k, _: start(res_copy, k), None)
        wait_bytes(line_maps.at[it, pl.ds(0, members - 1)], line_sem.at[it, 1])
        all_a, all_b = jnp.ones((tiles, LANES), F32), jnp.zeros((tiles, LANES), F32)
        own_a, own_b = all_a, all_b
        for k in range(members):
            step_a, step_b = line_maps[it, k, 0:tiles], line_maps[it, k, tiles : 2 * tiles]
            all_b = step_a * all_b + step_b
            all_a = step_a * all_a
            own_a = jnp.where(mine == k + 1, all_a, own_a)
            own_b = jnp.where(mine == k + 1, all_b, own_b)
        x_maps[it, x] = jnp.concatenate([all_a, all_b], 0)
        lax.fori_loop(1, nx, lambda k, _: start(functools.partial(x_copy, it), k), None)
        if sums is not None:
            wait_bytes(line_res.at[pl.ds(0, members - 1)], res_sem.at[1])
            plane_res[x * ny + y] = functools.reduce(
                jnp.add, [line_res[k] for k in range(members)]
            )
            lax.fori_loop(1, plane, lambda k, _: start(plane_copy, k), None)
        wait_bytes(x_maps.at[it, pl.ds(0, nx - 1)], x_sem.at[it, 1])
        held = lanes_to_rows(init_ref[...])
        for k in range(nx):
            step_a, step_b = x_maps[it, k, 0:tiles], x_maps[it, k, tiles : 2 * tiles]
            held = jnp.where(k < x, step_a * held + step_b, held)
        held = rows_to_lanes(own_a * held + own_b)
        return seg[0] * held + seg[1]

    def apply(p, enter):
        at = pl.ds(p * group, group)
        hist[pl.ds(1 + p * group, group)] = pre_a[at] * enter + pre_b[at]

    send_block(0, ORDER[0])
    table_copy.start()
    weight_copy.start()
    edge_copy.wait()
    first = lax.broadcasted_iota(jnp.int32, (SEGS, width), 0) == 0
    outer = jnp.where(tm == 0, jnp.broadcast_to(init_ref[...], (SEGS, width)), pltpu.roll(edge[...], 1, 0))
    hist[0] = jnp.where(first, outer, pltpu.roll(hist[steps], 1, 0))
    send_block(0, ORDER[1])
    send_block(0, 2)
    send_block(0, 3)

    table_copy.wait()

    def split(g, _):
        rest = table[g]
        for k in range(3):
            part = rest.astype(BF16)
            pieces[k, g] = part
            rest = rest - part.astype(F32)

    lax.fori_loop(0, 3, split, None)
    lane = lax.broadcasted_iota(jnp.int32, (SEGS, vocab), 1)

    def mark(k, _):
        ids = pltpu.roll(ids_ref[...], lax.rem(LANES - k * 8, LANES), 1)
        for u in range(0, 8, 2):
            both = [jnp.where(ids[:, v : v + 1] == lane, 1.0, 0.0) for v in (u, u + 1)]
            at = pl.ds(pl.multiple_of((k * 8 + u) * SEGS, 2 * SEGS), 2 * SEGS)
            onehot[at] = jnp.concatenate(both, 0).astype(BF16)

    lax.fori_loop(0, steps // 8, mark, None)

    def look_up(p, _):
        for g in range(3):
            found = dot(onehot[block_rows(p)], pieces[0, g])
            found += dot(onehot[block_rows(p)], pieces[1, g])
            found += dot(onehot[block_rows(p)], pieces[2, g])
            if g == 0:
                found += zb_ref[...]
            inp[g, block_rows(p)] = found

    lax.fori_loop(0, PAIRS, look_up, None)

    weight_copy.wait()
    same = lax.broadcasted_iota(jnp.int32, (LANES, LANES), 0) == lax.broadcasted_iota(
        jnp.int32, (LANES, LANES), 1
    )
    for g in range(3):
        for k in range(tiles):
            at = pl.ds(pl.multiple_of(y * width + k * LANES, LANES), LANES)
            corner = weight[g, at, k * LANES : (k + 1) * LANES].astype(F32)
            line = jnp.sum(jnp.where(same, corner, 0.0), 0, keepdims=True)
            diag[g, :, k * LANES : (k + 1) * LANES] = jnp.broadcast_to(line, (SEGS, LANES))

    run_a, run_b, first_err = sweep(0)
    enter = entering(0, run_a, run_b, None)
    hist[0] = enter
    for p in ORDER[:2][::-1]:
        apply(p, enter)
    for p in ORDER:
        if p > 1:
            apply(p, enter)
        send_block(1, p)
    first_sum = sum_tiles(first_err)

    run_a, run_b, second_err = sweep(1)
    second_sum = sum_tiles(second_err)
    enter = entering(1, run_a, run_b, (first_sum, second_sum))

    def out_copy(p, s):
        return pltpu.make_async_copy(
            hist.at[pl.ds(1 + p * group, group), s],
            out_hbm.at[pl.ds(s * steps + p * group, group)],
            out_sem.at[p, s],
        )

    for p in range(PAIRS):
        apply(p, enter)
        for s in range(SEGS):
            out_copy(p, s).start()
    wait_bytes(plane_res.at[pl.ds(0, plane - 1)], res_sem.at[3])
    sums = functools.reduce(jnp.add, [plane_res[k] for k in range(plane)])
    norms = jnp.sqrt(jnp.sum(sums, 1, keepdims=True) / count)
    for it in range(ITERS):
        res_ref[it] = norms[it, 0]

    for it in range(ITERS):
        wait_bytes(sent.at[it, pl.ds(0, 3)], send_sem.at[it])
        wait_bytes(line_maps.at[it, pl.ds(0, members - 1)], line_sem.at[it, 0])
        wait_bytes(x_maps.at[it, pl.ds(0, nx - 1)], x_sem.at[it, 0])
    wait_bytes(line_res.at[pl.ds(0, members - 1)], res_sem.at[0])
    wait_bytes(plane_res.at[pl.ds(0, plane - 1)], res_sem.at[2])
    for p in range(PAIRS):
        for s in range(SEGS):
            out_copy(p, s).wait()


def sum_tiles(err):
    return functools.reduce(
        jnp.add, [err[:, k : k + LANES] for k in range(0, err.shape[1], LANES)]
    )


def per_device(token_ids, input_table, recur_weight, z_bias, hn_bias, init_state, guess):
    rows, width = guess.shape
    vocab, full = input_table.shape[0], recur_weight.shape[0]
    nx, nz, nc, ny = (lax.axis_size(a) for a in (*TM, "hid"))
    steps, members, plane, tiles = rows // SEGS, nz * nc, nx * ny, width // LANES
    group = steps // PAIRS
    ids = token_ids.reshape(SEGS, steps)
    ids = jnp.concatenate([ids] * (LANES // steps), 1)
    anywhere = pl.BlockSpec(memory_space=pl.ANY)
    vmem = pl.BlockSpec(memory_space=pltpu.VMEM)
    sem = pltpu.SemaphoreType.DMA
    return pl.pallas_call(
        functools.partial(kernel, (nx, nz, nc, ny, rows, width, vocab)),
        out_shape=(
            jax.ShapeDtypeStruct((rows, width), F32),
            jax.ShapeDtypeStruct((ITERS,), F32),
        ),
        in_specs=[vmem, anywhere, anywhere, vmem, vmem, vmem, anywhere],
        out_specs=(anywhere, pl.BlockSpec(memory_space=pltpu.SMEM)),
        scratch_shapes=[
            pltpu.VMEM((3, vocab, width), F32),
            pltpu.VMEM((3, 3, vocab, width), BF16),
            pltpu.VMEM((3, full, width), BF16),
            pltpu.VMEM((steps + 1, SEGS, width), F32),
            pltpu.VMEM((ITERS, ny, rows, width), BF16),
            pltpu.VMEM((rows, vocab), BF16),
            pltpu.VMEM((3, rows, width), F32),
            pltpu.VMEM((3, rows, width), F32),
            pltpu.VMEM((steps, SEGS, width), F32),
            pltpu.VMEM((steps, SEGS, width), F32),
            pltpu.VMEM((3, SEGS, width), F32),
            pltpu.VMEM((2, SEGS, width), F32),
            pltpu.VMEM((SEGS, width), F32),
            pltpu.VMEM((ITERS, members, 2 * tiles, LANES), F32),
            pltpu.VMEM((ITERS, nx, 2 * tiles, LANES), F32),
            pltpu.VMEM((members, ITERS, LANES), F32),
            pltpu.VMEM((plane, ITERS, LANES), F32),
            sem((SEGS,)),
            sem((2,)),
            sem((PAIRS, SEGS)),
            sem((2,)),
            sem((ITERS,)),
            sem((ITERS, 2, PAIRS)),
            sem((ITERS, 2, PAIRS)),
            sem((ITERS, 2)),
            sem((ITERS, 2)),
            sem((4,)),
        ],
        compiler_params=pltpu.CompilerParams(
            collective_id=0, has_side_effects=True, vmem_limit_bytes=60 * 1024 * 1024
        ),
    )(
        ids,
        jnp.transpose(input_table, (1, 0, 2)),
        jnp.transpose(recur_weight, (1, 0, 2)),
        z_bias[None],
        hn_bias[None],
        init_state[None],
        guess,
    )


def solution(mesh):
    chips = mesh.devices.shape[0]
    nz, nc = (8, 2) if chips == 64 else (2, 2)
    finer = Mesh(
        mesh.devices.reshape(chips // (nz * nc), nz, nc, mesh.shape["hid"]), (*TM, "hid")
    )
    in_specs = (
        P(TM),
        P(None, None, "hid"),
        P(None, None, "hid"),
        P("hid"),
        P("hid"),
        P("hid"),
        P(TM, "hid"),
    )
    return jax.shard_map(
        per_device, mesh=finer, in_specs=in_specs, out_specs=(P(TM, "hid"), P()), check_vma=False
    )
```

```python
import functools

import jax
import jax.numpy as jnp
from jax import lax
from jax.experimental import pallas as pl
from jax.experimental.pallas import tpu as pltpu
from jax.sharding import Mesh
from jax.sharding import PartitionSpec as P

ITERS = 2
SEGS = 8
PAIRS = 4
LANES = 128
ORDER = (1, 0, 2, 3)
TM = ("tm_0", "tm_1", "tm_2")
MESH = pl.DeviceIdType.MESH
F32 = jnp.float32
BF16 = jnp.bfloat16


def dot(a, b):
    return jnp.dot(a, b, preferred_element_type=F32)


def sigmoid(x):
    return 0.5 * jnp.tanh(0.5 * x) + 0.5


def lanes_to_rows(row):
    return jnp.concatenate([row[:, k : k + LANES] for k in range(0, row.shape[1], LANES)], 0)


def rows_to_lanes(block):
    return jnp.concatenate([block[k : k + 1] for k in range(block.shape[0])], 1)


def wait_bytes(ref, sem):
    pltpu.make_async_copy(ref, ref, sem).wait()


def kernel(
    dims,
    ids_hbm,
    table_hbm,
    weight_hbm,
    zb_hbm,
    hb_hbm,
    init_hbm,
    guess_hbm,
    hist,
    plane_res,
    ids_ref,
    zb_ref,
    hb_ref,
    init_ref,
    table,
    pieces,
    weight,
    sent,
    onehot,
    inp,
    acc,
    pre_a,
    pre_b,
    diag,
    seg,
    edge,
    line_maps,
    x_maps,
    line_res,
    in_sem,
    weight_sem,
    edge_sem,
    send_sem,
    recv_sem,
    relay_sem,
    line_sem,
    x_sem,
    res_sem,
):
    nx, nz, nc, ny, rows, width, vocab = dims
    steps = rows // SEGS
    block = rows // PAIRS
    group = block // SEGS
    tiles = width // LANES
    members = nz * nc
    plane = nx * ny
    x, z, c, y = (lax.axis_index(a) for a in (*TM, "hid"))
    mine = z * nc + c
    tm = x * members + mine
    right, left, far = (lax.rem(y + d, ny) for d in (1, ny - 1, 2))

    def line_peer(k):
        k = members // 2 + k // 2 * (1 - 2 * lax.rem(k, 2))
        peer = lax.rem(mine + k, members)
        return {"tm_1": peer // nc, "tm_2": lax.rem(peer, nc)}

    def plane_peer(k):
        return {"tm_0": lax.rem(x + k // ny, nx), "hid": lax.rem(y + lax.rem(k, ny), ny)}

    def tm_peer(index):
        return {
            "tm_0": index // members,
            "tm_1": lax.rem(index, members) // nc,
            "tm_2": lax.rem(index, nc),
        }

    total = nx * members
    after, before = (lax.rem(tm + d, total) for d in (1, total - 1))

    barrier = pltpu.get_barrier_semaphore()

    def greet(peer):
        pl.semaphore_signal(barrier, inc=1, device_id=peer, device_id_type=MESH)

    greet(tm_peer(after))
    greet(tm_peer(before))
    lax.fori_loop(1, plane, lambda k, _: greet(plane_peer(k)), None)
    lax.fori_loop(1, members, lambda k, _: greet(line_peer(k)), None)

    for s in range(SEGS):
        pltpu.make_async_copy(
            guess_hbm.at[pl.ds(s * steps, steps)], hist.at[pl.ds(1, steps), s], in_sem.at[s]
        ).start()
    for s in range(SEGS):
        pltpu.make_async_copy(
            guess_hbm.at[pl.ds(s * steps, steps)], hist.at[pl.ds(1, steps), s], in_sem.at[s]
        ).wait()
    rows_copies = [
        pltpu.make_async_copy(source, target, in_sem.at[SEGS + k])
        for k, (source, target) in enumerate(
            ((ids_hbm, ids_ref), (zb_hbm, zb_ref), (hb_hbm, hb_ref), (init_hbm, init_ref))
        )
    ]
    for copy in rows_copies:
        copy.start()
    table_copy = pltpu.make_async_copy(table_hbm, table, weight_sem.at[0])
    weight_copy = pltpu.make_async_copy(weight_hbm, weight, weight_sem.at[1])
    pl.semaphore_wait(barrier, plane + members)

    edge_copy = pltpu.make_async_remote_copy(
        src_ref=hist.at[steps],
        dst_ref=edge,
        send_sem=edge_sem.at[0],
        recv_sem=edge_sem.at[1],
        device_id=tm_peer(after),
        device_id_type=MESH,
    )
    edge_copy.start()

    def piece(it, slot, p):
        return sent.at[it, slot, pl.ds(p * block, block)]

    def half(it, slot, p, h):
        return sent.at[it, slot, pl.ds(p * block + h * (block // 2), block // 2)]

    def direct(it, p, side, slot):
        return pltpu.make_async_remote_copy(
            src_ref=piece(it, slot, p),
            dst_ref=piece(it, slot, p),
            send_sem=send_sem.at[it],
            recv_sem=recv_sem.at[it, side, p],
            device_id={"hid": (right, left)[side]},
            device_id_type=MESH,
        )

    def relay(it, p, side, slot):
        return pltpu.make_async_remote_copy(
            src_ref=half(it, slot, p, side),
            dst_ref=half(it, slot, p, side),
            send_sem=send_sem.at[it],
            recv_sem=relay_sem.at[it, side, p],
            device_id={"hid": (right, left)[side]},
            device_id_type=MESH,
        )

    def block_rows(p):
        return pl.ds(pl.multiple_of(p * block, block), block)

    def weight_rows(slot):
        return pl.ds(pl.multiple_of(slot * width, width), width)

    def send_block(it, p):
        prev = hist[pl.ds(p * group, group)].reshape(block, width)
        sent[it, y, block_rows(p)] = prev.astype(BF16)
        direct(it, p, 0, y).start()
        direct(it, p, 1, y).start()

    def near_products(it):
        def visit(i, _):
            p = jnp.where(i < 2, 1 - i, i)
            direct(it, p, 0, left).wait_recv()
            relay(it, p, 0, left).start()
            direct(it, p, 1, right).wait_recv()
            relay(it, p, 1, right).start()

            def gate(g, _):
                part = dot(sent[it, y, block_rows(p)], weight[g, weight_rows(y)])
                part += dot(sent[it, left, block_rows(p)], weight[g, weight_rows(left)])
                part += dot(sent[it, right, block_rows(p)], weight[g, weight_rows(right)])
                acc[g, block_rows(p)] = part

            lax.fori_loop(0, 3, gate, None)

        lax.fori_loop(0, PAIRS, visit, None)

    def far_products(it, p):
        relay(it, p, 0, far).wait_recv()
        relay(it, p, 1, far).wait_recv()

        def gate(g, _):
            acc[g, block_rows(p)] += dot(sent[it, far, block_rows(p)], weight[g, weight_rows(far)])

        lax.fori_loop(0, 3, gate, None)

    def cells(it, p, carry):
        def visit(k, carry):
            run_a, run_b, err = carry
            j = p * group + k
            at = pl.ds(pl.multiple_of(j * SEGS, SEGS), SEGS)
            prev, state = hist[j], hist[j + 1]
            zeta = sigmoid(acc[0, at] + inp[0, at])
            reset = sigmoid(acc[1, at] + inp[1, at])
            cand_pre = acc[2, at] + hb_ref[...]
            cand = jnp.tanh(inp[2, at] + reset * cand_pre)
            moved = zeta * (prev - cand)
            value = cand + moved
            slope = reset * (diag[2] + cand_pre * (1.0 - reset) * diag[1])
            slope = moved * diag[0] + (1.0 - cand * cand) * slope
            slope = zeta + (1.0 - zeta) * slope
            gap = state - value
            run_a = slope * run_a
            run_b = slope * run_b + (value - slope * prev)
            pre_a[j] = run_a
            pre_b[j] = run_b
            return run_a, run_b, err + gap * gap

        return lax.fori_loop(0, group, visit, carry, unroll=2)

    def sweep(it):
        near_products(it)
        carry = (
            jnp.ones((SEGS, width), F32),
            jnp.zeros((SEGS, width), F32),
            jnp.zeros((SEGS, width), F32),
        )
        far_products(it, ORDER[0])
        far_products(it, ORDER[1])
        carry = cells(it, 0, carry)
        carry = cells(it, 1, carry)
        far_products(it, 2)
        carry = cells(it, 2, carry)
        far_products(it, 3)
        return cells(it, 3, carry)

    def line_copy(it, k):
        return pltpu.make_async_remote_copy(
            src_ref=line_maps.at[it, mine],
            dst_ref=line_maps.at[it, mine],
            send_sem=line_sem.at[it, 0],
            recv_sem=line_sem.at[it, 1],
            device_id=line_peer(k),
            device_id_type=MESH,
        )

    def x_copy(it, k):
        return pltpu.make_async_remote_copy(
            src_ref=x_maps.at[it, x],
            dst_ref=x_maps.at[it, x],
            send_sem=x_sem.at[it, 0],
            recv_sem=x_sem.at[it, 1],
            device_id={"tm_0": lax.rem(x + k, nx)},
            device_id_type=MESH,
        )

    def res_copy(k):
        return pltpu.make_async_remote_copy(
            src_ref=line_res.at[mine],
            dst_ref=line_res.at[mine],
            send_sem=res_sem.at[0],
            recv_sem=res_sem.at[1],
            device_id=line_peer(k),
            device_id_type=MESH,
        )

    def plane_copy(k):
        return pltpu.make_async_remote_copy(
            src_ref=plane_res.at[x * ny + y],
            dst_ref=plane_res.at[x * ny + y],
            send_sem=res_sem.at[2],
            recv_sem=res_sem.at[3],
            device_id=plane_peer(k),
            device_id_type=MESH,
        )

    def start(copy, k):
        copy(k).start()

    def entering(it, run_a, run_b, sums):
        if sums is not None:
            line_res[mine] = jnp.concatenate([jnp.sum(e, 0, keepdims=True) for e in sums], 0)
            lax.fori_loop(1, members, lambda k, _: start(res_copy, k), None)
        map_a, map_b = jnp.ones((1, width), F32), jnp.zeros((1, width), F32)
        for s in range(SEGS):
            seg[0, s : s + 1] = map_a
            seg[1, s : s + 1] = map_b
            map_b = run_a[s : s + 1] * map_b + run_b[s : s + 1]
            map_a = run_a[s : s + 1] * map_a
        line_maps[it, mine] = jnp.concatenate([lanes_to_rows(map_a), lanes_to_rows(map_b)], 0)
        lax.fori_loop(1, members, lambda k, _: start(functools.partial(line_copy, it), k), None)
        wait_bytes(line_maps.at[it, pl.ds(0, members - 1)], line_sem.at[it, 1])
        all_a, all_b = jnp.ones((tiles, LANES), F32), jnp.zeros((tiles, LANES), F32)
        own_a, own_b = all_a, all_b
        for k in range(members):
            step_a, step_b = line_maps[it, k, 0:tiles], line_maps[it, k, tiles : 2 * tiles]
            all_b = step_a * all_b + step_b
            all_a = step_a * all_a
            own_a = jnp.where(mine == k + 1, all_a, own_a)
            own_b = jnp.where(mine == k + 1, all_b, own_b)
        x_maps[it, x] = jnp.concatenate([all_a, all_b], 0)
        lax.fori_loop(1, nx, lambda k, _: start(functools.partial(x_copy, it), k), None)
        if sums is not None:
            wait_bytes(line_res.at[pl.ds(0, members - 1)], res_sem.at[1])
            plane_res[x * ny + y] = functools.reduce(
                jnp.add, [line_res[k] for k in range(members)]
            )
            lax.fori_loop(1, plane, lambda k, _: start(plane_copy, k), None)
        wait_bytes(x_maps.at[it, pl.ds(0, nx - 1)], x_sem.at[it, 1])
        held = lanes_to_rows(init_ref[...])
        for k in range(nx):
            step_a, step_b = x_maps[it, k, 0:tiles], x_maps[it, k, tiles : 2 * tiles]
            held = jnp.where(k < x, step_a * held + step_b, held)
        held = rows_to_lanes(own_a * held + own_b)
        return seg[0] * held + seg[1]

    def apply(p, enter):
        at = pl.ds(p * group, group)
        hist[pl.ds(1 + p * group, group)] = pre_a[at] * enter + pre_b[at]

    send_block(0, ORDER[0])
    table_copy.start()
    weight_copy.start()
    for copy in rows_copies:
        copy.wait()
    edge_copy.wait()
    first = lax.broadcasted_iota(jnp.int32, (SEGS, width), 0) == 0
    outer = jnp.where(tm == 0, jnp.broadcast_to(init_ref[...], (SEGS, width)), pltpu.roll(edge[...], 1, 0))
    hist[0] = jnp.where(first, outer, pltpu.roll(hist[steps], 1, 0))
    send_block(0, ORDER[1])
    send_block(0, 2)
    send_block(0, 3)

    table_copy.wait()

    def split(g, _):
        rest = table[g]
        for k in range(3):
            part = rest.astype(BF16)
            pieces[k, g] = part
            rest = rest - part.astype(F32)

    lax.fori_loop(0, 3, split, None)
    lane = lax.broadcasted_iota(jnp.int32, (SEGS, vocab), 1)
    lines = []
    for s in range(SEGS):
        tile = s * steps // LANES * LANES
        line = ids_ref[:, tile : tile + LANES]
        back = s * steps - tile
        lines.append(pltpu.roll(line, LANES - back, 1) if back else line)
    by_segment = jnp.concatenate(lines, 0)

    def mark(k, _):
        ids = pltpu.roll(by_segment, lax.rem(LANES - k * 8, LANES), 1)
        for u in range(0, 8, 2):
            both = [jnp.where(ids[:, v : v + 1] == lane, 1.0, 0.0) for v in (u, u + 1)]
            at = pl.ds(pl.multiple_of((k * 8 + u) * SEGS, 2 * SEGS), 2 * SEGS)
            onehot[at] = jnp.concatenate(both, 0).astype(BF16)

    lax.fori_loop(0, steps // 8, mark, None)

    def look_up(p, _):
        for g in range(3):
            found = dot(onehot[block_rows(p)], pieces[0, g])
            found += dot(onehot[block_rows(p)], pieces[1, g])
            found += dot(onehot[block_rows(p)], pieces[2, g])
            if g == 0:
                found += zb_ref[...]
            inp[g, block_rows(p)] = found

    lax.fori_loop(0, PAIRS, look_up, None)

    weight_copy.wait()
    same = lax.broadcasted_iota(jnp.int32, (LANES, LANES), 0) == lax.broadcasted_iota(
        jnp.int32, (LANES, LANES), 1
    )
    for g in range(3):
        for k in range(tiles):
            at = pl.ds(pl.multiple_of(y * width + k * LANES, LANES), LANES)
            corner = weight[g, at, k * LANES : (k + 1) * LANES].astype(F32)
            line = jnp.sum(jnp.where(same, corner, 0.0), 0, keepdims=True)
            diag[g, :, k * LANES : (k + 1) * LANES] = jnp.broadcast_to(line, (SEGS, LANES))

    run_a, run_b, first_err = sweep(0)
    enter = entering(0, run_a, run_b, None)
    hist[0] = enter
    for p in ORDER[:2][::-1]:
        apply(p, enter)
    for p in ORDER:
        if p > 1:
            apply(p, enter)
        send_block(1, p)
    first_sum = sum_tiles(first_err)

    run_a, run_b, second_err = sweep(1)
    second_sum = sum_tiles(second_err)
    enter = entering(1, run_a, run_b, (first_sum, second_sum))

    for p in range(PAIRS):
        apply(p, enter)
    wait_bytes(plane_res.at[pl.ds(0, plane - 1)], res_sem.at[3])

    for it in range(ITERS):
        wait_bytes(sent.at[it, pl.ds(0, 3)], send_sem.at[it])
        wait_bytes(line_maps.at[it, pl.ds(0, members - 1)], line_sem.at[it, 0])
        wait_bytes(x_maps.at[it, pl.ds(0, nx - 1)], x_sem.at[it, 0])
    wait_bytes(line_res.at[pl.ds(0, members - 1)], res_sem.at[0])
    wait_bytes(plane_res.at[pl.ds(0, plane - 1)], res_sem.at[2])


def write_out(count, hist, plane_res, out_hbm, res_ref, out_sem):
    steps = hist.shape[0] - 1
    copies = [
        pltpu.make_async_copy(
            hist.at[pl.ds(1, steps), s], out_hbm.at[pl.ds(s * steps, steps)], out_sem.at[s]
        )
        for s in range(SEGS)
    ]
    for copy in copies:
        copy.start()
    sums = functools.reduce(jnp.add, [plane_res[k] for k in range(plane_res.shape[0])])
    norms = jnp.sqrt(jnp.sum(sums, 1, keepdims=True) / count)
    for it in range(ITERS):
        res_ref[it] = norms[it, 0]
    for copy in copies:
        copy.wait()


def sum_tiles(err):
    return functools.reduce(
        jnp.add, [err[:, k : k + LANES] for k in range(0, err.shape[1], LANES)]
    )


def per_device(token_ids, input_table, recur_weight, z_bias, hn_bias, init_state, guess):
    rows, width = guess.shape
    vocab, full = input_table.shape[0], recur_weight.shape[0]
    nx, nz, nc, ny = (lax.axis_size(a) for a in (*TM, "hid"))
    steps, members, plane, tiles = rows // SEGS, nz * nc, nx * ny, width // LANES
    group = steps // PAIRS
    anywhere = pl.BlockSpec(memory_space=pl.ANY)
    vmem = pl.BlockSpec(memory_space=pltpu.VMEM)
    sem = pltpu.SemaphoreType.DMA
    hist, plane_res = pl.pallas_call(
        functools.partial(kernel, (nx, nz, nc, ny, rows, width, vocab)),
        out_shape=(
            pltpu.VMEM((steps + 1, SEGS, width), F32),
            pltpu.VMEM((plane, ITERS, LANES), F32),
        ),
        in_specs=[pl.BlockSpec(memory_space=pltpu.HBM)] * 7,
        out_specs=(vmem, vmem),
        scratch_shapes=[
            pltpu.VMEM((1, rows), jnp.int32),
            pltpu.VMEM((1, width), F32),
            pltpu.VMEM((1, width), F32),
            pltpu.VMEM((1, width), F32),
            pltpu.VMEM((3, vocab, width), F32),
            pltpu.VMEM((3, 3, vocab, width), BF16),
            pltpu.VMEM((3, full, width), BF16),
            pltpu.VMEM((ITERS, ny, rows, width), BF16),
            pltpu.VMEM((rows, vocab), BF16),
            pltpu.VMEM((3, rows, width), F32),
            pltpu.VMEM((3, rows, width), F32),
            pltpu.VMEM((steps, SEGS, width), F32),
            pltpu.VMEM((steps, SEGS, width), F32),
            pltpu.VMEM((3, SEGS, width), F32),
            pltpu.VMEM((2, SEGS, width), F32),
            pltpu.VMEM((SEGS, width), F32),
            pltpu.VMEM((ITERS, members, 2 * tiles, LANES), F32),
            pltpu.VMEM((ITERS, nx, 2 * tiles, LANES), F32),
            pltpu.VMEM((members, ITERS, LANES), F32),
            sem((SEGS + 4,)),
            sem((2,)),
            sem((2,)),
            sem((ITERS,)),
            sem((ITERS, 2, PAIRS)),
            sem((ITERS, 2, PAIRS)),
            sem((ITERS, 2)),
            sem((ITERS, 2)),
            sem((4,)),
        ],
        compiler_params=pltpu.CompilerParams(
            collective_id=0, has_side_effects=True, vmem_limit_bytes=40 * 1024 * 1024
        ),
    )(
        *(
            pltpu.with_memory_space_constraint(array, pltpu.HBM)
            for array in (
                token_ids[None],
                jnp.transpose(input_table, (1, 0, 2)),
                jnp.transpose(recur_weight, (1, 0, 2)),
                z_bias[None],
                hn_bias[None],
                init_state[None],
                guess,
            )
        )
    )
    return pl.pallas_call(
        functools.partial(write_out, nx * members * rows * ny * width),
        out_shape=(
            jax.ShapeDtypeStruct((rows, width), F32),
            jax.ShapeDtypeStruct((ITERS,), F32),
        ),
        in_specs=[vmem, vmem],
        out_specs=(anywhere, pl.BlockSpec(memory_space=pltpu.SMEM)),
        scratch_shapes=[sem((SEGS,))],
        compiler_params=pltpu.CompilerParams(vmem_limit_bytes=8 * 1024 * 1024),
    )(hist, plane_res)


def solution(mesh):
    chips = mesh.devices.shape[0]
    nz, nc = (8, 2) if chips == 64 else (2, 2)
    finer = Mesh(
        mesh.devices.reshape(chips // (nz * nc), nz, nc, mesh.shape["hid"]), (*TM, "hid")
    )
    in_specs = (
        P(TM),
        P(None, None, "hid"),
        P(None, None, "hid"),
        P("hid"),
        P("hid"),
        P("hid"),
        P(TM, "hid"),
    )
    return jax.shard_map(
        per_device, mesh=finer, in_specs=in_specs, out_specs=(P(TM, "hid"), P()), check_vma=False
    )
```

```python
import functools

import jax
import jax.numpy as jnp
from jax import lax
from jax.experimental import pallas as pl
from jax.experimental.pallas import tpu as pltpu
from jax.sharding import Mesh
from jax.sharding import PartitionSpec as P

ITERS = 2
SEGS = 8
PAIRS = 4
LANES = 128
ORDERS = ((1, 0, 2, 3), (0, 1, 2, 3))
TM = ("tm_0", "tm_1", "tm_2")
MESH = pl.DeviceIdType.MESH
F32 = jnp.float32
BF16 = jnp.bfloat16


def dot(a, b):
    return jnp.dot(a, b, preferred_element_type=F32)


def sigmoid(x):
    return 0.5 * jnp.tanh(0.5 * x) + 0.5


def lanes_to_rows(row):
    return jnp.concatenate([row[:, k : k + LANES] for k in range(0, row.shape[1], LANES)], 0)


def rows_to_lanes(block):
    return jnp.concatenate([block[k : k + 1] for k in range(block.shape[0])], 1)


def wait_bytes(ref, sem):
    pltpu.make_async_copy(ref, ref, sem).wait()


def kernel(
    dims,
    ids_hbm,
    table_hbm,
    weight_hbm,
    zb_hbm,
    hb_hbm,
    init_hbm,
    guess_hbm,
    hist,
    sums_ref,
    ids_ref,
    zb_ref,
    hb_ref,
    init_ref,
    table,
    pieces,
    weight,
    sent,
    onehot,
    inp,
    acc,
    pre_a,
    pre_b,
    diag,
    seg,
    edge,
    own_map,
    twin_map,
    z_maps,
    x_maps,
    enter_row,
    here,
    own_res,
    twin_res,
    z_res,
    plane_res,
    sum_row,
    in_sem,
    weight_sem,
    edge_sem,
    send_sem,
    recv_sem,
    relay_sem,
    map_sem,
    z_sem,
    x_sem,
    enter_sem,
    res_sem,
):
    nx, nz, nc, ny, rows, width, vocab = dims
    steps = rows // SEGS
    block = rows // PAIRS
    group = block // SEGS
    tiles = width // LANES
    members = nz * nc
    plane = nx * ny
    x, z, c, y = (lax.axis_index(a) for a in (*TM, "hid"))
    tm = x * members + z * nc + c
    twin = {"tm_2": 1 - c}
    right, left, far = (lax.rem(y + d, ny) for d in (1, ny - 1, 2))

    def far_first(k, size):
        return size // 2 + k // 2 * (1 - 2 * lax.rem(k, 2))

    def z_peer(k):
        return {"tm_1": lax.rem(z + far_first(k, nz), nz)}

    def x_peer(k):
        return {"tm_0": lax.rem(x + far_first(k, nx), nx)}

    def each(count, act):
        lax.fori_loop(1, count, lambda k, _: act(k), None)

    def plane_peer(k):
        return {"tm_0": lax.rem(x + k // ny, nx), "hid": lax.rem(y + lax.rem(k, ny), ny)}

    def tm_peer(index):
        return {
            "tm_0": index // members,
            "tm_1": lax.rem(index, members) // nc,
            "tm_2": lax.rem(index, nc),
        }

    total = nx * members
    after, before = (lax.rem(tm + d, total) for d in (1, total - 1))

    barrier = pltpu.get_barrier_semaphore()

    def greet(peer):
        pl.semaphore_signal(barrier, inc=1, device_id=peer, device_id_type=MESH)

    greet(tm_peer(after))
    greet(tm_peer(before))
    greet(twin)
    each(plane, lambda k: greet(plane_peer(k)))
    each(nz, lambda k: greet(z_peer(k)))

    for s in range(SEGS):
        pltpu.make_async_copy(
            guess_hbm.at[pl.ds(s * steps, steps)], hist.at[pl.ds(1, steps), s], in_sem.at[s]
        ).start()
    for s in range(SEGS):
        pltpu.make_async_copy(
            guess_hbm.at[pl.ds(s * steps, steps)], hist.at[pl.ds(1, steps), s], in_sem.at[s]
        ).wait()
    rows_copies = [
        pltpu.make_async_copy(source, target, in_sem.at[SEGS + k])
        for k, (source, target) in enumerate(
            ((ids_hbm, ids_ref), (zb_hbm, zb_ref), (hb_hbm, hb_ref), (init_hbm, init_ref))
        )
    ]
    for copy in rows_copies:
        copy.start()
    table_copy = pltpu.make_async_copy(table_hbm, table, weight_sem.at[0])
    weight_copy = pltpu.make_async_copy(weight_hbm, weight, weight_sem.at[1])
    pl.semaphore_wait(barrier, plane + nz + 1)

    edge_copy = pltpu.make_async_remote_copy(
        src_ref=hist.at[steps],
        dst_ref=edge,
        send_sem=edge_sem.at[0],
        recv_sem=edge_sem.at[1],
        device_id=tm_peer(after),
        device_id_type=MESH,
    )
    edge_copy.start()

    def piece(it, slot, p):
        return sent.at[it, slot, pl.ds(p * block, block)]

    def half(it, slot, p, h):
        return sent.at[it, slot, pl.ds(p * block + h * (block // 2), block // 2)]

    def direct(it, p, side, slot):
        return pltpu.make_async_remote_copy(
            src_ref=piece(it, slot, p),
            dst_ref=piece(it, slot, p),
            send_sem=send_sem.at[it],
            recv_sem=recv_sem.at[it, side, p],
            device_id={"hid": (right, left)[side]},
            device_id_type=MESH,
        )

    def relay(it, p, side, slot):
        return pltpu.make_async_remote_copy(
            src_ref=half(it, slot, p, side),
            dst_ref=half(it, slot, p, side),
            send_sem=send_sem.at[it],
            recv_sem=relay_sem.at[it, side, p],
            device_id={"hid": (right, left)[side]},
            device_id_type=MESH,
        )

    def block_rows(p):
        return pl.ds(pl.multiple_of(p * block, block), block)

    def weight_rows(slot):
        return pl.ds(pl.multiple_of(slot * width, width), width)

    def send_block(it, p):
        prev = hist[pl.ds(p * group, group)].reshape(block, width)
        sent[it, y, block_rows(p)] = prev.astype(BF16)
        direct(it, p, 0, y).start()
        direct(it, p, 1, y).start()

    def near_products(it):
        def visit(i, _):
            p = jnp.where(i < 2, 1 - i, i) if it == 0 else i
            direct(it, p, 0, left).wait_recv()
            relay(it, p, 0, left).start()
            direct(it, p, 1, right).wait_recv()
            relay(it, p, 1, right).start()

            def gate(g, _):
                part = dot(sent[it, y, block_rows(p)], weight[g, weight_rows(y)])
                part += dot(sent[it, left, block_rows(p)], weight[g, weight_rows(left)])
                part += dot(sent[it, right, block_rows(p)], weight[g, weight_rows(right)])
                acc[g, block_rows(p)] = part

            lax.fori_loop(0, 3, gate, None)

        lax.fori_loop(0, PAIRS, visit, None)

    def far_products(it, p):
        relay(it, p, 0, far).wait_recv()
        relay(it, p, 1, far).wait_recv()

        for g in range(3):
            acc[g, block_rows(p)] += dot(sent[it, far, block_rows(p)], weight[g, weight_rows(far)])

    def cells(it, p, carry):
        def visit(k, carry):
            run_a, run_b, err = carry
            j = p * group + k
            at = pl.ds(pl.multiple_of(j * SEGS, SEGS), SEGS)
            prev, state = hist[j], hist[j + 1]
            zeta = sigmoid(acc[0, at] + inp[0, at])
            reset = sigmoid(acc[1, at] + inp[1, at])
            cand_pre = acc[2, at] + hb_ref[...]
            cand = jnp.tanh(inp[2, at] + reset * cand_pre)
            moved = zeta * (prev - cand)
            value = cand + moved
            slope = reset * (diag[2] + cand_pre * (1.0 - reset) * diag[1])
            slope = moved * diag[0] + (1.0 - cand * cand) * slope
            slope = zeta + (1.0 - zeta) * slope
            gap = state - value
            run_a = slope * run_a
            run_b = slope * run_b + (value - slope * prev)
            pre_a[j] = run_a
            pre_b[j] = run_b
            return run_a, run_b, err + gap * gap

        return lax.fori_loop(0, group, visit, carry, unroll=2)

    def sweep(it):
        near_products(it)
        carry = (
            jnp.ones((SEGS, width), F32),
            jnp.zeros((SEGS, width), F32),
            jnp.zeros((SEGS, width), F32),
        )
        ready = 0
        for i, p in enumerate(ORDERS[it]):
            far_products(it, p)
            while ready in ORDERS[it][: i + 1]:
                carry = cells(it, ready, carry)
                ready += 1
        return carry

    def send(ref, target, sems, peer):
        return pltpu.make_async_remote_copy(
            src_ref=ref,
            dst_ref=target,
            send_sem=sems.at[0],
            recv_sem=sems.at[1],
            device_id=peer,
            device_id_type=MESH,
        )

    def map_copy(it):
        return send(own_map.at[it], twin_map.at[it], map_sem.at[it], twin)

    def z_copy(it, k):
        return send(z_maps.at[it, z], z_maps.at[it, z], z_sem.at[it], z_peer(k))

    def x_copy(it, k):
        return send(x_maps.at[it, x], x_maps.at[it, x], x_sem.at[it], x_peer(k))

    def enter_copy(it):
        return send(enter_row.at[it], enter_row.at[it], enter_sem.at[it], twin)

    def twin_res_copy():
        return send(own_res, twin_res, res_sem.at[0], twin)

    def z_res_copy(k):
        return send(z_res.at[z], z_res.at[z], res_sem.at[1], z_peer(k))

    def plane_copy(k):
        slot = plane_res.at[x * ny + y]
        return send(slot, slot, res_sem.at[2], plane_peer(k))

    def sum_copy():
        return send(sum_row, sum_row, res_sem.at[3], twin)

    def halves(block):
        return block[0:tiles], block[tiles : 2 * tiles]

    def entering(it, run_a, run_b, sums):
        if sums is not None:
            own_res[...] = jnp.concatenate([jnp.sum(e, 0, keepdims=True) for e in sums], 0)

            @pl.when(c == 0)
            def _():
                twin_res_copy().start()

        map_a, map_b = jnp.ones((1, width), F32), jnp.zeros((1, width), F32)
        for s in range(SEGS):
            seg[0, s : s + 1] = map_a
            seg[1, s : s + 1] = map_b
            map_b = run_a[s : s + 1] * map_b + run_b[s : s + 1]
            map_a = run_a[s : s + 1] * map_a
        own_map[it] = jnp.concatenate([lanes_to_rows(map_a), lanes_to_rows(map_b)], 0)

        @pl.when(c == 0)
        def _():
            map_copy(it).start()
            enter_copy(it).wait_recv()
            here[...] = enter_row[it]

        @pl.when(c == 1)
        def _():
            map_copy(it).wait_recv()
            twin_a, twin_b = halves(twin_map[it])
            last_a, last_b = halves(own_map[it])
            z_maps[it, z] = jnp.concatenate([last_a * twin_a, last_a * twin_b + last_b], 0)
            each(nz, lambda k: z_copy(it, k).start())
            if sums is not None:
                twin_res_copy().wait_recv()
                z_res[z] = own_res[...] + twin_res[...]
                each(nz, lambda k: z_res_copy(k).start())
            wait_bytes(z_maps.at[it, pl.ds(0, nz - 1)], z_sem.at[it, 1])
            all_a, all_b = jnp.ones((tiles, LANES), F32), jnp.zeros((tiles, LANES), F32)
            own_a, own_b = all_a, all_b
            for k in range(nz):
                step_a, step_b = halves(z_maps[it, k])
                all_b = step_a * all_b + step_b
                all_a = step_a * all_a
                own_a = jnp.where(z == k + 1, all_a, own_a)
                own_b = jnp.where(z == k + 1, all_b, own_b)
            x_maps[it, x] = jnp.concatenate([all_a, all_b], 0)
            each(nx, lambda k: x_copy(it, k).start())
            if sums is not None:
                wait_bytes(z_res.at[pl.ds(0, nz - 1)], res_sem.at[1, 1])
                plane_res[x * ny + y] = functools.reduce(jnp.add, [z_res[k] for k in range(nz)])
                each(plane, lambda k: plane_copy(k).start())
            wait_bytes(x_maps.at[it, pl.ds(0, nx - 1)], x_sem.at[it, 1])
            held = lanes_to_rows(init_ref[...])
            for k in range(nx):
                step_a, step_b = halves(x_maps[it, k])
                held = jnp.where(k < x, step_a * held + step_b, held)
            held = own_a * held + own_b
            enter_row[it] = held
            enter_copy(it).start()
            here[...] = twin_a * held + twin_b

        return seg[0] * rows_to_lanes(here[...]) + seg[1]

    def apply(p, enter):
        at = pl.ds(p * group, group)
        hist[pl.ds(1 + p * group, group)] = pre_a[at] * enter + pre_b[at]

    send_block(0, ORDERS[0][0])
    table_copy.start()
    weight_copy.start()
    for copy in rows_copies:
        copy.wait()
    edge_copy.wait()
    first = lax.broadcasted_iota(jnp.int32, (SEGS, width), 0) == 0
    outer = jnp.where(tm == 0, jnp.broadcast_to(init_ref[...], (SEGS, width)), pltpu.roll(edge[...], 1, 0))
    hist[0] = jnp.where(first, outer, pltpu.roll(hist[steps], 1, 0))
    for p in ORDERS[0][1:]:
        send_block(0, p)

    table_copy.wait()

    def split(g, _):
        rest = table[g]
        for k in range(3):
            part = rest.astype(BF16)
            pieces[k, g] = part
            rest = rest - part.astype(F32)

    lax.fori_loop(0, 3, split, None)
    lane = lax.broadcasted_iota(jnp.int32, (SEGS, vocab), 1)
    lines = []
    for s in range(SEGS):
        tile = s * steps // LANES * LANES
        line = ids_ref[:, tile : tile + LANES]
        back = s * steps - tile
        lines.append(pltpu.roll(line, LANES - back, 1) if back else line)
    by_segment = jnp.concatenate(lines, 0)

    def mark(k, _):
        ids = pltpu.roll(by_segment, lax.rem(LANES - k * 8, LANES), 1)
        for u in range(0, 8, 2):
            both = [jnp.where(ids[:, v : v + 1] == lane, 1.0, 0.0) for v in (u, u + 1)]
            at = pl.ds(pl.multiple_of((k * 8 + u) * SEGS, 2 * SEGS), 2 * SEGS)
            onehot[at] = jnp.concatenate(both, 0).astype(BF16)

    lax.fori_loop(0, steps // 8, mark, None)

    def look_up(p, _):
        for g in range(3):
            found = dot(onehot[block_rows(p)], pieces[0, g])
            found += dot(onehot[block_rows(p)], pieces[1, g])
            found += dot(onehot[block_rows(p)], pieces[2, g])
            if g == 0:
                found += zb_ref[...]
            inp[g, block_rows(p)] = found

    lax.fori_loop(0, PAIRS, look_up, None)

    weight_copy.wait()
    same = lax.broadcasted_iota(jnp.int32, (LANES, LANES), 0) == lax.broadcasted_iota(
        jnp.int32, (LANES, LANES), 1
    )
    for g in range(3):
        for k in range(tiles):
            at = pl.ds(pl.multiple_of(y * width + k * LANES, LANES), LANES)
            corner = weight[g, at, k * LANES : (k + 1) * LANES].astype(F32)
            line = jnp.sum(jnp.where(same, corner, 0.0), 0, keepdims=True)
            diag[g, :, k * LANES : (k + 1) * LANES] = jnp.broadcast_to(line, (SEGS, LANES))

    run_a, run_b, first_err = sweep(0)
    enter = entering(0, run_a, run_b, None)
    hist[0] = enter
    for p in ORDERS[1]:
        apply(p, enter)
        send_block(1, p)
    first_sum = sum_tiles(first_err)

    run_a, run_b, second_err = sweep(1)
    second_sum = sum_tiles(second_err)
    enter = entering(1, run_a, run_b, (first_sum, second_sum))

    for p in range(PAIRS):
        apply(p, enter)

    @pl.when(c == 1)
    def _():
        wait_bytes(plane_res.at[pl.ds(0, plane - 1)], res_sem.at[2, 1])
        sum_row[...] = functools.reduce(jnp.add, [plane_res[k] for k in range(plane)])
        sum_copy().start()
        for it in range(ITERS):
            wait_bytes(z_maps.at[it, pl.ds(0, nz - 1)], z_sem.at[it, 0])
            wait_bytes(x_maps.at[it, pl.ds(0, nx - 1)], x_sem.at[it, 0])
            enter_copy(it).wait_send()
        wait_bytes(z_res.at[pl.ds(0, nz - 1)], res_sem.at[1, 0])
        wait_bytes(plane_res.at[pl.ds(0, plane - 1)], res_sem.at[2, 0])
        sum_copy().wait_send()

    @pl.when(c == 0)
    def _():
        for it in range(ITERS):
            map_copy(it).wait_send()
        twin_res_copy().wait_send()
        sum_copy().wait_recv()

    sums_ref[...] = sum_row[...]
    for it in range(ITERS):
        wait_bytes(sent.at[it, pl.ds(0, 3)], send_sem.at[it])


def write_out(count, hist, sums_ref, out_hbm, res_ref, out_sem):
    steps = hist.shape[0] - 1
    copies = [
        pltpu.make_async_copy(
            hist.at[pl.ds(1, steps), s], out_hbm.at[pl.ds(s * steps, steps)], out_sem.at[s]
        )
        for s in range(SEGS)
    ]
    for copy in copies:
        copy.start()
    norms = jnp.sqrt(jnp.sum(sums_ref[...], 1, keepdims=True) / count)
    for it in range(ITERS):
        res_ref[it] = norms[it, 0]
    for copy in copies:
        copy.wait()


def sum_tiles(err):
    return functools.reduce(
        jnp.add, [err[:, k : k + LANES] for k in range(0, err.shape[1], LANES)]
    )


def per_device(token_ids, input_table, recur_weight, z_bias, hn_bias, init_state, guess):
    rows, width = guess.shape
    vocab, full = input_table.shape[0], recur_weight.shape[0]
    nx, nz, nc, ny = (lax.axis_size(a) for a in (*TM, "hid"))
    steps, plane, tiles = rows // SEGS, nx * ny, width // LANES
    anywhere = pl.BlockSpec(memory_space=pl.ANY)
    vmem = pl.BlockSpec(memory_space=pltpu.VMEM)
    sem = pltpu.SemaphoreType.DMA
    hist, sums = pl.pallas_call(
        functools.partial(kernel, (nx, nz, nc, ny, rows, width, vocab)),
        out_shape=(
            pltpu.VMEM((steps + 1, SEGS, width), F32),
            pltpu.VMEM((ITERS, LANES), F32),
        ),
        in_specs=[pl.BlockSpec(memory_space=pltpu.HBM)] * 7,
        out_specs=(vmem, vmem),
        scratch_shapes=[
            pltpu.VMEM((1, rows), jnp.int32),
            pltpu.VMEM((1, width), F32),
            pltpu.VMEM((1, width), F32),
            pltpu.VMEM((1, width), F32),
            pltpu.VMEM((3, vocab, width), F32),
            pltpu.VMEM((3, 3, vocab, width), BF16),
            pltpu.VMEM((3, full, width), BF16),
            pltpu.VMEM((ITERS, ny, rows, width), BF16),
            pltpu.VMEM((rows, vocab), BF16),
            pltpu.VMEM((3, rows, width), F32),
            pltpu.VMEM((3, rows, width), F32),
            pltpu.VMEM((steps, SEGS, width), F32),
            pltpu.VMEM((steps, SEGS, width), F32),
            pltpu.VMEM((3, SEGS, width), F32),
            pltpu.VMEM((2, SEGS, width), F32),
            pltpu.VMEM((SEGS, width), F32),
            pltpu.VMEM((ITERS, 2 * tiles, LANES), F32),
            pltpu.VMEM((ITERS, 2 * tiles, LANES), F32),
            pltpu.VMEM((ITERS, nz, 2 * tiles, LANES), F32),
            pltpu.VMEM((ITERS, nx, 2 * tiles, LANES), F32),
            pltpu.VMEM((ITERS, tiles, LANES), F32),
            pltpu.VMEM((tiles, LANES), F32),
            pltpu.VMEM((ITERS, LANES), F32),
            pltpu.VMEM((ITERS, LANES), F32),
            pltpu.VMEM((nz, ITERS, LANES), F32),
            pltpu.VMEM((plane, ITERS, LANES), F32),
            pltpu.VMEM((ITERS, LANES), F32),
            sem((SEGS + 4,)),
            sem((2,)),
            sem((2,)),
            sem((ITERS,)),
            sem((ITERS, 2, PAIRS)),
            sem((ITERS, 2, PAIRS)),
            sem((ITERS, 2)),
            sem((ITERS, 2)),
            sem((ITERS, 2)),
            sem((ITERS, 2)),
            sem((4, 2)),
        ],
        compiler_params=pltpu.CompilerParams(
            collective_id=0, has_side_effects=True, vmem_limit_bytes=40 * 1024 * 1024
        ),
    )(
        *(
            pltpu.with_memory_space_constraint(array, pltpu.HBM)
            for array in (
                token_ids[None],
                jnp.transpose(input_table, (1, 0, 2)),
                jnp.transpose(recur_weight, (1, 0, 2)),
                z_bias[None],
                hn_bias[None],
                init_state[None],
                guess,
            )
        )
    )
    return pl.pallas_call(
        functools.partial(write_out, nx * nz * nc * rows * ny * width),
        out_shape=(
            jax.ShapeDtypeStruct((rows, width), F32),
            jax.ShapeDtypeStruct((ITERS,), F32),
        ),
        in_specs=[vmem, vmem],
        out_specs=(anywhere, pl.BlockSpec(memory_space=pltpu.SMEM)),
        scratch_shapes=[sem((SEGS,))],
        compiler_params=pltpu.CompilerParams(vmem_limit_bytes=8 * 1024 * 1024),
    )(hist, sums)


def solution(mesh):
    chips = mesh.devices.shape[0]
    nz, nc = (8, 2) if chips == 64 else (2, 2)
    finer = Mesh(
        mesh.devices.reshape(chips // (nz * nc), nz, nc, mesh.shape["hid"]), (*TM, "hid")
    )
    in_specs = (
        P(TM),
        P(None, None, "hid"),
        P(None, None, "hid"),
        P("hid"),
        P("hid"),
        P("hid"),
        P(TM, "hid"),
    )
    return jax.shard_map(
        per_device, mesh=finer, in_specs=in_specs, out_specs=(P(TM, "hid"), P()), check_vma=False
    )
```

```python
import functools

import jax
import jax.numpy as jnp
from jax import lax
from jax.experimental import pallas as pl
from jax.experimental.pallas import tpu as pltpu
from jax.sharding import Mesh
from jax.sharding import PartitionSpec as P

ITERS = 2
SEGS = 8
BLOCKS = 4
LANES = 128
ORDERS = ((1, 0, 2, 3), tuple(range(BLOCKS)))
TM = ("tm_0", "tm_1", "tm_2")
MESH = pl.DeviceIdType.MESH
F32 = jnp.float32
BF16 = jnp.bfloat16


def dot(a, b):
    return jnp.dot(a, b, preferred_element_type=F32)


def sigmoid(x):
    return 0.5 * jnp.tanh(0.5 * x) + 0.5


def lanes_to_rows(row):
    return jnp.concatenate([row[:, k : k + LANES] for k in range(0, row.shape[1], LANES)], 0)


def rows_to_lanes(block):
    return jnp.concatenate([block[k : k + 1] for k in range(block.shape[0])], 1)


def wait_bytes(ref, sem):
    pltpu.make_async_copy(ref, ref, sem).wait()


def kernel(
    dims,
    ids_hbm,
    table_hbm,
    weight_hbm,
    zb_hbm,
    hb_hbm,
    init_hbm,
    guess_hbm,
    hist,
    sums_ref,
    ids_ref,
    zb_ref,
    hb_ref,
    init_ref,
    table,
    pieces,
    weight,
    sent,
    onehot,
    inp,
    acc,
    pre_a,
    pre_b,
    diag,
    seg,
    edge,
    z_maps,
    x_maps,
    enter_row,
    here,
    z_res,
    plane_res,
    sum_row,
    in_sem,
    weight_sem,
    edge_sem,
    send_sem,
    recv_sem,
    relay_sem,
    z_sem,
    x_sem,
    enter_sem,
    res_sem,
):
    nx, nz, nc, ny, rows, width, vocab = dims
    steps = rows // SEGS
    block = rows // BLOCKS
    group = block // SEGS
    tiles = width // LANES
    members = nz * nc
    plane = nx * ny
    x, z, c, y = (lax.axis_index(a) for a in (*TM, "hid"))
    tm = x * members + z * nc + c
    mine = z * nc + c
    twin = {"tm_2": 1 - c}
    right, left, far = (lax.rem(y + d, ny) for d in (1, ny - 1, 2))

    def far_first(k, size):
        return size // 2 + k // 2 * (1 - 2 * lax.rem(k, 2))

    def z_peer(k, core):
        return {"tm_1": lax.rem(z + far_first(k, nz), nz), "tm_2": core}

    def x_peer(k):
        return {"tm_0": lax.rem(x + far_first(k, nx), nx)}

    def each(count, act):
        lax.fori_loop(1, count, lambda k, _: act(k), None)

    def plane_peer(k):
        return {"tm_0": lax.rem(x + k // ny, nx), "hid": lax.rem(y + lax.rem(k, ny), ny)}

    def tm_peer(index):
        return {
            "tm_0": index // members,
            "tm_1": lax.rem(index, members) // nc,
            "tm_2": lax.rem(index, nc),
        }

    total = nx * members
    after, before = (lax.rem(tm + d, total) for d in (1, total - 1))

    barrier = pltpu.get_barrier_semaphore()

    def greet(peer):
        pl.semaphore_signal(barrier, inc=1, device_id=peer, device_id_type=MESH)

    greet(tm_peer(after))
    greet(tm_peer(before))
    greet(twin)
    each(plane, lambda k: greet(plane_peer(k)))
    for core in range(nc):
        each(nz, lambda k: greet(z_peer(k, core)))

    for s in range(SEGS):
        pltpu.make_async_copy(
            guess_hbm.at[pl.ds(s * steps, steps)], hist.at[pl.ds(1, steps), s], in_sem.at[s]
        ).start()
    for s in range(SEGS):
        pltpu.make_async_copy(
            guess_hbm.at[pl.ds(s * steps, steps)], hist.at[pl.ds(1, steps), s], in_sem.at[s]
        ).wait()
    rows_copies = [
        pltpu.make_async_copy(source, target, in_sem.at[SEGS + k])
        for k, (source, target) in enumerate(
            ((ids_hbm, ids_ref), (zb_hbm, zb_ref), (hb_hbm, hb_ref), (init_hbm, init_ref))
        )
    ]
    for copy in rows_copies:
        copy.start()
    table_copy = pltpu.make_async_copy(table_hbm, table, weight_sem.at[0])
    weight_copy = pltpu.make_async_copy(weight_hbm, weight, weight_sem.at[1])
    pl.semaphore_wait(barrier, plane + 2 + nc * (nz - 1))

    edge_copy = pltpu.make_async_remote_copy(
        src_ref=hist.at[steps],
        dst_ref=edge,
        send_sem=edge_sem.at[0],
        recv_sem=edge_sem.at[1],
        device_id=tm_peer(after),
        device_id_type=MESH,
    )
    edge_copy.start()

    def piece(it, slot, p):
        return sent.at[it, slot, pl.ds(p * block, block)]

    def half(it, slot, p, h):
        return sent.at[it, slot, pl.ds(p * block + h * (block // 2), block // 2)]

    def direct(it, p, side, slot):
        return pltpu.make_async_remote_copy(
            src_ref=piece(it, slot, p),
            dst_ref=piece(it, slot, p),
            send_sem=send_sem.at[it],
            recv_sem=recv_sem.at[it, side, p],
            device_id={"hid": (right, left)[side]},
            device_id_type=MESH,
        )

    def relay(it, p, side, slot):
        return pltpu.make_async_remote_copy(
            src_ref=half(it, slot, p, side),
            dst_ref=half(it, slot, p, side),
            send_sem=send_sem.at[it],
            recv_sem=relay_sem.at[it, side, p],
            device_id={"hid": (right, left)[side]},
            device_id_type=MESH,
        )

    def block_rows(p):
        return pl.ds(pl.multiple_of(p * block, block), block)

    def weight_rows(slot):
        return pl.ds(pl.multiple_of(slot * width, width), width)

    def send_block(it, p):
        prev = hist[pl.ds(p * group, group)].reshape(block, width)
        sent[it, y, block_rows(p)] = prev.astype(BF16)
        direct(it, p, 0, y).start()
        direct(it, p, 1, y).start()

    def near_products(it):
        def visit(i, _):
            p = jnp.where(i < 2, 1 - i, i) if it == 0 else i
            direct(it, p, 0, left).wait_recv()
            relay(it, p, 0, left).start()
            direct(it, p, 1, right).wait_recv()
            relay(it, p, 1, right).start()

            def gate(g, _):
                part = dot(sent[it, y, block_rows(p)], weight[g, weight_rows(y)])
                part += dot(sent[it, left, block_rows(p)], weight[g, weight_rows(left)])
                part += dot(sent[it, right, block_rows(p)], weight[g, weight_rows(right)])
                acc[g, block_rows(p)] = part

            lax.fori_loop(0, 3, gate, None)

        lax.fori_loop(0, BLOCKS, visit, None)

    def far_products(it, p):
        relay(it, p, 0, far).wait_recv()
        relay(it, p, 1, far).wait_recv()

        for g in range(3):
            acc[g, block_rows(p)] += dot(sent[it, far, block_rows(p)], weight[g, weight_rows(far)])

    def cells(it, p, carry):
        def visit(k, carry):
            run_a, run_b, err = carry
            j = p * group + k
            at = pl.ds(pl.multiple_of(j * SEGS, SEGS), SEGS)
            prev, state = hist[j], hist[j + 1]
            zeta = sigmoid(acc[0, at] + inp[0, at])
            reset = sigmoid(acc[1, at] + inp[1, at])
            cand_pre = acc[2, at] + hb_ref[...]
            cand = jnp.tanh(inp[2, at] + reset * cand_pre)
            moved = zeta * (prev - cand)
            value = cand + moved
            slope = reset * (diag[2] + cand_pre * (1.0 - reset) * diag[1])
            slope = moved * diag[0] + (1.0 - cand * cand) * slope
            slope = zeta + (1.0 - zeta) * slope
            gap = state - value
            run_a = slope * run_a
            run_b = slope * run_b + (value - slope * prev)
            pre_a[j] = run_a
            pre_b[j] = run_b
            return run_a, run_b, err + gap * gap

        return lax.fori_loop(0, group, visit, carry, unroll=2)

    def sweep(it):
        near_products(it)
        carry = (
            jnp.ones((SEGS, width), F32),
            jnp.zeros((SEGS, width), F32),
            jnp.zeros((SEGS, width), F32),
        )
        ready = 0
        for i, p in enumerate(ORDERS[it]):
            far_products(it, p)
            while ready in ORDERS[it][: i + 1]:
                carry = cells(it, ready, carry)
                ready += 1
        return carry

    def send(ref, target, sems, peer):
        return pltpu.make_async_remote_copy(
            src_ref=ref,
            dst_ref=target,
            send_sem=sems.at[0],
            recv_sem=sems.at[1],
            device_id=peer,
            device_id_type=MESH,
        )

    def to_line(slot, sems):
        each(nz, lambda k: send(slot, slot, sems, z_peer(k, 1)).start())

        @pl.when(c == 0)
        def _():
            send(slot, slot, sems, twin).start()

    def x_copy(it, k):
        return send(x_maps.at[it, x], x_maps.at[it, x], x_sem.at[it], x_peer(k))

    def enter_copy(it):
        return send(enter_row.at[it], enter_row.at[it], enter_sem.at[it], twin)

    def plane_copy(k):
        slot = plane_res.at[x * ny + y]
        return send(slot, slot, res_sem.at[2], plane_peer(k))

    def sum_copy():
        return send(sum_row, sum_row, res_sem.at[3], twin)

    def halves(block):
        return block[0:tiles], block[tiles : 2 * tiles]

    def entering(it, run_a, run_b, sums):
        if sums is not None:
            z_res[mine] = jnp.concatenate([jnp.sum(e, 0, keepdims=True) for e in sums], 0)
            to_line(z_res.at[mine], res_sem.at[1])
        map_a, map_b = jnp.ones((1, width), F32), jnp.zeros((1, width), F32)
        for s in range(SEGS):
            seg[0, s : s + 1] = map_a
            seg[1, s : s + 1] = map_b
            map_b = run_a[s : s + 1] * map_b + run_b[s : s + 1]
            map_a = run_a[s : s + 1] * map_a
        z_maps[it, mine] = jnp.concatenate([lanes_to_rows(map_a), lanes_to_rows(map_b)], 0)
        to_line(z_maps.at[it, mine], z_sem.at[it])

        @pl.when(c == 0)
        def _():
            enter_copy(it).wait_recv()
            here[...] = enter_row[it]

        @pl.when(c == 1)
        def _():
            if sums is not None:
                wait_bytes(z_res.at[pl.ds(0, members - 1)], res_sem.at[1, 1])
                plane_res[x * ny + y] = functools.reduce(
                    jnp.add, [z_res[k] for k in range(members)]
                )
                each(plane, lambda k: plane_copy(k).start())
            wait_bytes(z_maps.at[it, pl.ds(0, members - 1)], z_sem.at[it, 1])
            all_a, all_b = jnp.ones((tiles, LANES), F32), jnp.zeros((tiles, LANES), F32)
            own_a, own_b = all_a, all_b
            for k in range(members):
                step_a, step_b = halves(z_maps[it, k])
                all_b = step_a * all_b + step_b
                all_a = step_a * all_a
                if k % nc == nc - 1:
                    own_a = jnp.where(mine == k + nc, all_a, own_a)
                    own_b = jnp.where(mine == k + nc, all_b, own_b)
            x_maps[it, x] = jnp.concatenate([all_a, all_b], 0)
            each(nx, lambda k: x_copy(it, k).start())
            wait_bytes(x_maps.at[it, pl.ds(0, nx - 1)], x_sem.at[it, 1])
            held = lanes_to_rows(init_ref[...])
            for k in range(nx):
                step_a, step_b = halves(x_maps[it, k])
                held = jnp.where(k < x, step_a * held + step_b, held)
            held = own_a * held + own_b
            enter_row[it] = held
            enter_copy(it).start()
            twin_a, twin_b = halves(z_maps[it, z * nc])
            here[...] = twin_a * held + twin_b

        return seg[0] * rows_to_lanes(here[...]) + seg[1]

    def apply(p, enter):
        at = pl.ds(p * group, group)
        hist[pl.ds(1 + p * group, group)] = pre_a[at] * enter + pre_b[at]

    send_block(0, ORDERS[0][0])
    table_copy.start()
    weight_copy.start()
    for copy in rows_copies:
        copy.wait()
    edge_copy.wait()
    first = lax.broadcasted_iota(jnp.int32, (SEGS, width), 0) == 0
    outer = jnp.where(tm == 0, jnp.broadcast_to(init_ref[...], (SEGS, width)), pltpu.roll(edge[...], 1, 0))
    hist[0] = jnp.where(first, outer, pltpu.roll(hist[steps], 1, 0))
    for p in ORDERS[0][1:]:
        send_block(0, p)

    table_copy.wait()

    def split(g, _):
        rest = table[g]
        for k in range(3):
            part = rest.astype(BF16)
            pieces[k, g] = part
            rest = rest - part.astype(F32)

    lax.fori_loop(0, 3, split, None)
    lane = lax.broadcasted_iota(jnp.int32, (SEGS, vocab), 1)
    lines = []
    for s in range(SEGS):
        tile = s * steps // LANES * LANES
        line = ids_ref[:, tile : tile + LANES]
        back = s * steps - tile
        lines.append(pltpu.roll(line, LANES - back, 1) if back else line)
    by_segment = jnp.concatenate(lines, 0)

    def mark(k, _):
        ids = pltpu.roll(by_segment, lax.rem(LANES - k * 8, LANES), 1)
        for u in range(0, 8, 2):
            both = [jnp.where(ids[:, v : v + 1] == lane, 1.0, 0.0) for v in (u, u + 1)]
            at = pl.ds(pl.multiple_of((k * 8 + u) * SEGS, 2 * SEGS), 2 * SEGS)
            onehot[at] = jnp.concatenate(both, 0).astype(BF16)

    lax.fori_loop(0, steps // 8, mark, None)

    def look_up(p, _):
        for g in range(3):
            found = dot(onehot[block_rows(p)], pieces[0, g])
            found += dot(onehot[block_rows(p)], pieces[1, g])
            found += dot(onehot[block_rows(p)], pieces[2, g])
            if g == 0:
                found += zb_ref[...]
            inp[g, block_rows(p)] = found

    lax.fori_loop(0, BLOCKS, look_up, None)

    weight_copy.wait()
    same = lax.broadcasted_iota(jnp.int32, (LANES, LANES), 0) == lax.broadcasted_iota(
        jnp.int32, (LANES, LANES), 1
    )
    for g in range(3):
        for k in range(tiles):
            at = pl.ds(pl.multiple_of(y * width + k * LANES, LANES), LANES)
            corner = weight[g, at, k * LANES : (k + 1) * LANES].astype(F32)
            line = jnp.sum(jnp.where(same, corner, 0.0), 0, keepdims=True)
            diag[g, :, k * LANES : (k + 1) * LANES] = jnp.broadcast_to(line, (SEGS, LANES))

    run_a, run_b, first_err = sweep(0)
    enter = entering(0, run_a, run_b, None)
    hist[0] = enter
    for p in ORDERS[1]:
        apply(p, enter)
        send_block(1, p)
    first_sum = sum_tiles(first_err)

    run_a, run_b, second_err = sweep(1)
    second_sum = sum_tiles(second_err)
    enter = entering(1, run_a, run_b, (first_sum, second_sum))

    for p in range(BLOCKS):
        apply(p, enter)

    @pl.when(c == 1)
    def _():
        wait_bytes(plane_res.at[pl.ds(0, plane - 1)], res_sem.at[2, 1])
        sum_row[...] = functools.reduce(jnp.add, [plane_res[k] for k in range(plane)])
        sum_copy().start()
        for it in range(ITERS):
            wait_bytes(z_maps.at[it, pl.ds(0, nz - 1)], z_sem.at[it, 0])
            wait_bytes(x_maps.at[it, pl.ds(0, nx - 1)], x_sem.at[it, 0])
            enter_copy(it).wait_send()
        wait_bytes(z_res.at[pl.ds(0, nz - 1)], res_sem.at[1, 0])
        wait_bytes(plane_res.at[pl.ds(0, plane - 1)], res_sem.at[2, 0])
        sum_copy().wait_send()

    @pl.when(c == 0)
    def _():
        for it in range(ITERS):
            wait_bytes(z_maps.at[it, pl.ds(0, nz)], z_sem.at[it, 0])
        wait_bytes(z_res.at[pl.ds(0, nz)], res_sem.at[1, 0])
        sum_copy().wait_recv()

    sums_ref[...] = sum_row[...]
    for it in range(ITERS):
        wait_bytes(sent.at[it, pl.ds(0, 3)], send_sem.at[it])


def write_out(count, hist, sums_ref, out_hbm, res_ref, out_sem):
    steps = hist.shape[0] - 1
    copies = [
        pltpu.make_async_copy(
            hist.at[pl.ds(1, steps), s], out_hbm.at[pl.ds(s * steps, steps)], out_sem.at[s]
        )
        for s in range(SEGS)
    ]
    for copy in copies:
        copy.start()
    norms = jnp.sqrt(jnp.sum(sums_ref[...], 1, keepdims=True) / count)
    for it in range(ITERS):
        res_ref[it] = norms[it, 0]
    for copy in copies:
        copy.wait()


def sum_tiles(err):
    return functools.reduce(
        jnp.add, [err[:, k : k + LANES] for k in range(0, err.shape[1], LANES)]
    )


def per_device(token_ids, input_table, recur_weight, z_bias, hn_bias, init_state, guess):
    rows, width = guess.shape
    vocab, full = input_table.shape[0], recur_weight.shape[0]
    nx, nz, nc, ny = (lax.axis_size(a) for a in (*TM, "hid"))
    steps, plane, tiles = rows // SEGS, nx * ny, width // LANES
    anywhere = pl.BlockSpec(memory_space=pl.ANY)
    vmem = pl.BlockSpec(memory_space=pltpu.VMEM)
    sem = pltpu.SemaphoreType.DMA
    hist, sums = pl.pallas_call(
        functools.partial(kernel, (nx, nz, nc, ny, rows, width, vocab)),
        out_shape=(
            pltpu.VMEM((steps + 1, SEGS, width), F32),
            pltpu.VMEM((ITERS, LANES), F32),
        ),
        in_specs=[pl.BlockSpec(memory_space=pltpu.HBM)] * 7,
        out_specs=(vmem, vmem),
        scratch_shapes=[
            pltpu.VMEM((1, rows), jnp.int32),
            pltpu.VMEM((1, width), F32),
            pltpu.VMEM((1, width), F32),
            pltpu.VMEM((1, width), F32),
            pltpu.VMEM((3, vocab, width), F32),
            pltpu.VMEM((3, 3, vocab, width), BF16),
            pltpu.VMEM((3, full, width), BF16),
            pltpu.VMEM((ITERS, ny, rows, width), BF16),
            pltpu.VMEM((rows, vocab), BF16),
            pltpu.VMEM((3, rows, width), F32),
            pltpu.VMEM((3, rows, width), F32),
            pltpu.VMEM((steps, SEGS, width), F32),
            pltpu.VMEM((steps, SEGS, width), F32),
            pltpu.VMEM((3, SEGS, width), F32),
            pltpu.VMEM((2, SEGS, width), F32),
            pltpu.VMEM((SEGS, width), F32),
            pltpu.VMEM((ITERS, nz * nc, 2 * tiles, LANES), F32),
            pltpu.VMEM((ITERS, nx, 2 * tiles, LANES), F32),
            pltpu.VMEM((ITERS, tiles, LANES), F32),
            pltpu.VMEM((tiles, LANES), F32),
            pltpu.VMEM((nz * nc, ITERS, LANES), F32),
            pltpu.VMEM((plane, ITERS, LANES), F32),
            pltpu.VMEM((ITERS, LANES), F32),
            sem((SEGS + 4,)),
            sem((2,)),
            sem((2,)),
            sem((ITERS,)),
            sem((ITERS, 2, BLOCKS)),
            sem((ITERS, 2, BLOCKS)),
            sem((ITERS, 2)),
            sem((ITERS, 2)),
            sem((ITERS, 2)),
            sem((4, 2)),
        ],
        compiler_params=pltpu.CompilerParams(
            collective_id=0, has_side_effects=True, vmem_limit_bytes=40 * 1024 * 1024
        ),
    )(
        *(
            pltpu.with_memory_space_constraint(array, pltpu.HBM)
            for array in (
                token_ids[None],
                jnp.transpose(input_table, (1, 0, 2)),
                jnp.transpose(recur_weight, (1, 0, 2)),
                z_bias[None],
                hn_bias[None],
                init_state[None],
                guess,
            )
        )
    )
    return pl.pallas_call(
        functools.partial(write_out, nx * nz * nc * rows * ny * width),
        out_shape=(
            jax.ShapeDtypeStruct((rows, width), F32),
            jax.ShapeDtypeStruct((ITERS,), F32),
        ),
        in_specs=[vmem, vmem],
        out_specs=(anywhere, pl.BlockSpec(memory_space=pltpu.SMEM)),
        scratch_shapes=[sem((SEGS,))],
        compiler_params=pltpu.CompilerParams(vmem_limit_bytes=8 * 1024 * 1024),
    )(hist, sums)


def solution(mesh):
    chips = mesh.devices.shape[0]
    nz, nc = (8, 2) if chips == 64 else (2, 2)
    finer = Mesh(
        mesh.devices.reshape(chips // (nz * nc), nz, nc, mesh.shape["hid"]), (*TM, "hid")
    )
    in_specs = (
        P(TM),
        P(None, None, "hid"),
        P(None, None, "hid"),
        P("hid"),
        P("hid"),
        P("hid"),
        P(TM, "hid"),
    )
    return jax.shard_map(
        per_device, mesh=finer, in_specs=in_specs, out_specs=(P(TM, "hid"), P()), check_vma=False
    )
```

```python
import functools

import jax
import jax.numpy as jnp
from jax import lax
from jax.experimental import pallas as pl
from jax.experimental.pallas import tpu as pltpu
from jax.sharding import Mesh
from jax.sharding import PartitionSpec as P

ITERS = 2
SEGS = 8
BLOCKS = 4
LANES = 128
ORDERS = ((1, 0, 2, 3), tuple(range(BLOCKS)))
TM = ("tm_0", "tm_1", "tm_2")
MESH = pl.DeviceIdType.MESH
F32 = jnp.float32
BF16 = jnp.bfloat16


def dot(a, b):
    return jnp.dot(a, b, preferred_element_type=F32)


def sigmoid(x):
    return 0.5 * jnp.tanh(0.5 * x) + 0.5


def lanes_to_rows(row):
    return jnp.concatenate([row[:, k : k + LANES] for k in range(0, row.shape[1], LANES)], 0)


def rows_to_lanes(block):
    return jnp.concatenate([block[k : k + 1] for k in range(block.shape[0])], 1)


def wait_bytes(ref, sem):
    pltpu.make_async_copy(ref, ref, sem).wait()


def kernel(
    dims,
    ids_hbm,
    table_hbm,
    weight_hbm,
    zb_hbm,
    hb_hbm,
    init_hbm,
    guess_hbm,
    hist,
    sums_ref,
    ids_ref,
    zb_ref,
    hb_ref,
    init_ref,
    table,
    pieces,
    weight,
    sent,
    onehot,
    inp,
    acc,
    pre_a,
    pre_b,
    diag,
    seg,
    edge,
    z_maps,
    x_maps,
    enter_row,
    here,
    z_res,
    plane_res,
    sum_row,
    lead_maps,
    enters,
    in_sem,
    weight_sem,
    edge_sem,
    send_sem,
    recv_sem,
    relay_sem,
    z_sem,
    x_sem,
    enter_sem,
    res_sem,
    lead_sem,
):
    nx, nz, nc, ny, rows, width, vocab = dims
    steps = rows // SEGS
    block = rows // BLOCKS
    group = block // SEGS
    lead = rows // 16
    lead_steps = lead // SEGS - 1
    tiles = width // LANES
    members = nz * nc
    plane = nx * ny
    x, z, c, y = (lax.axis_index(a) for a in (*TM, "hid"))
    tm = x * members + z * nc + c
    mine = z * nc + c
    twin = {"tm_2": 1 - c}
    right, left, far = (lax.rem(y + d, ny) for d in (1, ny - 1, 2))

    def far_first(k, size):
        return size // 2 + k // 2 * (1 - 2 * lax.rem(k, 2))

    def z_peer(k, core):
        return {"tm_1": lax.rem(z + far_first(k, nz), nz), "tm_2": core}

    def x_peer(k):
        return {"tm_0": lax.rem(x + far_first(k, nx), nx)}

    def each(count, act):
        lax.fori_loop(1, count, lambda k, _: act(k), None)

    def plane_peer(k):
        return {"tm_0": lax.rem(x + k // ny, nx), "hid": lax.rem(y + lax.rem(k, ny), ny)}

    def tm_peer(index):
        return {
            "tm_0": index // members,
            "tm_1": lax.rem(index, members) // nc,
            "tm_2": lax.rem(index, nc),
        }

    total = nx * members
    after, before = (lax.rem(tm + d, total) for d in (1, total - 1))

    barrier = pltpu.get_barrier_semaphore()

    def greet(peer):
        pl.semaphore_signal(barrier, inc=1, device_id=peer, device_id_type=MESH)

    greet(tm_peer(after))
    greet(tm_peer(before))
    greet(twin)
    each(plane, lambda k: greet(plane_peer(k)))
    for core in range(nc):
        each(nz, lambda k: greet(z_peer(k, core)))

    for s in range(SEGS):
        pltpu.make_async_copy(
            guess_hbm.at[pl.ds(s * steps, steps)], hist.at[pl.ds(1, steps), s], in_sem.at[s]
        ).start()
    for s in range(SEGS):
        pltpu.make_async_copy(
            guess_hbm.at[pl.ds(s * steps, steps)], hist.at[pl.ds(1, steps), s], in_sem.at[s]
        ).wait()
    rows_copies = [
        pltpu.make_async_copy(source, target, in_sem.at[SEGS + k])
        for k, (source, target) in enumerate(
            ((ids_hbm, ids_ref), (zb_hbm, zb_ref), (hb_hbm, hb_ref), (init_hbm, init_ref))
        )
    ]
    for copy in rows_copies:
        copy.start()
    table_copy = pltpu.make_async_copy(table_hbm, table, weight_sem.at[0])
    weight_copy = pltpu.make_async_copy(weight_hbm, weight, weight_sem.at[1])
    pl.semaphore_wait(barrier, plane + 2 + nc * (nz - 1))

    edge_copy = pltpu.make_async_remote_copy(
        src_ref=hist.at[steps],
        dst_ref=edge,
        send_sem=edge_sem.at[0],
        recv_sem=edge_sem.at[1],
        device_id=tm_peer(after),
        device_id_type=MESH,
    )
    edge_copy.start()

    def piece(it, slot, p):
        skip = lead if it and isinstance(p, int) and p == 0 else 0
        return sent.at[it, slot, pl.ds(p * block + skip, block - skip)]

    def half(it, slot, p, h):
        skip = lead if it and isinstance(p, int) and p == 0 else 0
        size = (block - skip) // 2
        return sent.at[it, slot, pl.ds(p * block + skip + h * size, size)]

    def lead_copy(part, side, slot):
        source = (pre_a, pre_b)[part].at[pl.ds(0, lead_steps)]
        return pltpu.make_async_remote_copy(
            src_ref=source,
            dst_ref=lead_maps.at[slot, part],
            send_sem=lead_sem.at[0],
            recv_sem=lead_sem.at[2 + 2 * side + part],
            device_id={"hid": (right, left)[side]},
            device_id_type=MESH,
        )

    def lead_relay(side, slot):
        return pltpu.make_async_remote_copy(
            src_ref=lead_maps.at[slot, side],
            dst_ref=lead_maps.at[slot, side],
            send_sem=lead_sem.at[0],
            recv_sem=lead_sem.at[6 + side],
            device_id={"hid": (right, left)[side]},
            device_id_type=MESH,
        )

    def lead_enter(k, slot):
        return pltpu.make_async_remote_copy(
            src_ref=enters.at[slot],
            dst_ref=enters.at[slot],
            send_sem=lead_sem.at[1],
            recv_sem=lead_sem.at[8 + k],
            device_id={"hid": (right, left, far)[k]},
            device_id_type=MESH,
        )

    def start_lead():
        for side in range(2):
            for part in range(2):
                lead_copy(part, side, y).start()

    def forward_lead():
        for side, slot in ((0, left), (1, right)):
            for part in range(2):
                lead_copy(part, side, slot).wait_recv()
            lead_relay(side, slot).start()

    def fill_lead():
        for side in range(2):
            lead_relay(side, far).wait_recv()
        for k, slot in enumerate((left, right, far)):
            lead_enter(k, slot).wait_recv()
            state = enters[slot]
            prev = [state] + [
                lead_maps[slot, 0, j] * state + lead_maps[slot, 1, j] for j in range(lead_steps)
            ]
            sent[1, slot, 0:lead] = jnp.concatenate(prev, 0).astype(BF16)

    def direct(it, p, side, slot):
        return pltpu.make_async_remote_copy(
            src_ref=piece(it, slot, p),
            dst_ref=piece(it, slot, p),
            send_sem=send_sem.at[it],
            recv_sem=recv_sem.at[it, side, p],
            device_id={"hid": (right, left)[side]},
            device_id_type=MESH,
        )

    def relay(it, p, side, slot):
        return pltpu.make_async_remote_copy(
            src_ref=half(it, slot, p, side),
            dst_ref=half(it, slot, p, side),
            send_sem=send_sem.at[it],
            recv_sem=relay_sem.at[it, side, p],
            device_id={"hid": (right, left)[side]},
            device_id_type=MESH,
        )

    def block_rows(p):
        return pl.ds(pl.multiple_of(p * block, block), block)

    def weight_rows(slot):
        return pl.ds(pl.multiple_of(slot * width, width), width)

    def send_block(it, p):
        prev = hist[pl.ds(p * group, group)].reshape(block, width)
        sent[it, y, block_rows(p)] = prev.astype(BF16)
        direct(it, p, 0, y).start()
        direct(it, p, 1, y).start()

    def near_products(it):
        def visit(p, _):
            direct(it, p, 0, left).wait_recv()
            relay(it, p, 0, left).start()
            direct(it, p, 1, right).wait_recv()
            relay(it, p, 1, right).start()
            if it and isinstance(p, int):
                fill_lead()

            def gate(g, _):
                part = dot(sent[it, y, block_rows(p)], weight[g, weight_rows(y)])
                part += dot(sent[it, left, block_rows(p)], weight[g, weight_rows(left)])
                part += dot(sent[it, right, block_rows(p)], weight[g, weight_rows(right)])
                acc[g, block_rows(p)] = part

            lax.fori_loop(0, 3, gate, None)

        if it:
            visit(0, None)
            lax.fori_loop(1, BLOCKS, visit, None)
            wait_bytes(lead_maps.at[pl.ds(0, 3)], lead_sem.at[0])
        else:
            lax.fori_loop(0, BLOCKS, lambda i, _: visit(jnp.where(i < 2, 1 - i, i), None), None)

    def far_products(it, p):
        relay(it, p, 0, far).wait_recv()
        relay(it, p, 1, far).wait_recv()

        for g in range(3):
            acc[g, block_rows(p)] += dot(sent[it, far, block_rows(p)], weight[g, weight_rows(far)])

    def cells(it, p, carry):
        def visit(k, carry):
            run_a, run_b, err = carry
            j = p * group + k
            at = pl.ds(pl.multiple_of(j * SEGS, SEGS), SEGS)
            prev, state = hist[j], hist[j + 1]
            zeta = sigmoid(acc[0, at] + inp[0, at])
            reset = sigmoid(acc[1, at] + inp[1, at])
            cand_pre = acc[2, at] + hb_ref[...]
            cand = jnp.tanh(inp[2, at] + reset * cand_pre)
            moved = zeta * (prev - cand)
            value = cand + moved
            slope = reset * (diag[2] + cand_pre * (1.0 - reset) * diag[1])
            slope = moved * diag[0] + (1.0 - cand * cand) * slope
            slope = zeta + (1.0 - zeta) * slope
            gap = state - value
            run_a = slope * run_a
            run_b = slope * run_b + (value - slope * prev)
            pre_a[j] = run_a
            pre_b[j] = run_b
            return run_a, run_b, err + gap * gap

        return lax.fori_loop(0, group, visit, carry, unroll=2)

    def sweep(it):
        near_products(it)
        carry = (
            jnp.ones((SEGS, width), F32),
            jnp.zeros((SEGS, width), F32),
            jnp.zeros((SEGS, width), F32),
        )
        ready = 0
        for i, p in enumerate(ORDERS[it]):
            far_products(it, p)
            while ready in ORDERS[it][: i + 1]:
                carry = cells(it, ready, carry)
                ready += 1
        return carry

    def send(ref, target, sems, peer):
        return pltpu.make_async_remote_copy(
            src_ref=ref,
            dst_ref=target,
            send_sem=sems.at[0],
            recv_sem=sems.at[1],
            device_id=peer,
            device_id_type=MESH,
        )

    def to_line(slot, sems):
        each(nz, lambda k: send(slot, slot, sems, z_peer(k, 1)).start())

        @pl.when(c == 0)
        def _():
            send(slot, slot, sems, twin).start()

    def x_copy(it, k):
        return send(x_maps.at[it, x], x_maps.at[it, x], x_sem.at[it], x_peer(k))

    def enter_copy(it):
        return send(enter_row.at[it], enter_row.at[it], enter_sem.at[it], twin)

    def plane_copy(k):
        slot = plane_res.at[x * ny + y]
        return send(slot, slot, res_sem.at[2], plane_peer(k))

    def sum_copy():
        return send(sum_row, sum_row, res_sem.at[3], twin)

    def halves(block):
        return block[0:tiles], block[tiles : 2 * tiles]

    def entering(it, run_a, run_b, sums):
        if sums is not None:
            z_res[mine] = jnp.concatenate([jnp.sum(e, 0, keepdims=True) for e in sums], 0)
            to_line(z_res.at[mine], res_sem.at[1])
        map_a, map_b = jnp.ones((1, width), F32), jnp.zeros((1, width), F32)
        for s in range(SEGS):
            seg[0, s : s + 1] = map_a
            seg[1, s : s + 1] = map_b
            map_b = run_a[s : s + 1] * map_b + run_b[s : s + 1]
            map_a = run_a[s : s + 1] * map_a
        z_maps[it, mine] = jnp.concatenate([lanes_to_rows(map_a), lanes_to_rows(map_b)], 0)
        to_line(z_maps.at[it, mine], z_sem.at[it])
        if sums is None:
            start_lead()

        @pl.when(c == 0)
        def _():
            if sums is None:
                forward_lead()
            enter_copy(it).wait_recv()
            here[...] = enter_row[it]

        @pl.when(c == 1)
        def _():
            if sums is not None:
                wait_bytes(z_res.at[pl.ds(0, members - 1)], res_sem.at[1, 1])
                plane_res[x * ny + y] = functools.reduce(
                    jnp.add, [z_res[k] for k in range(members)]
                )
                each(plane, lambda k: plane_copy(k).start())
            wait_bytes(z_maps.at[it, pl.ds(0, members - 1)], z_sem.at[it, 1])
            all_a, all_b = jnp.ones((tiles, LANES), F32), jnp.zeros((tiles, LANES), F32)
            own_a, own_b = all_a, all_b
            for k in range(members):
                step_a, step_b = halves(z_maps[it, k])
                all_b = step_a * all_b + step_b
                all_a = step_a * all_a
                if k % nc == nc - 1:
                    own_a = jnp.where(mine == k + nc, all_a, own_a)
                    own_b = jnp.where(mine == k + nc, all_b, own_b)
            x_maps[it, x] = jnp.concatenate([all_a, all_b], 0)
            each(nx, lambda k: x_copy(it, k).start())
            if sums is None:
                forward_lead()
            wait_bytes(x_maps.at[it, pl.ds(0, nx - 1)], x_sem.at[it, 1])
            held = lanes_to_rows(init_ref[...])
            for k in range(nx):
                step_a, step_b = halves(x_maps[it, k])
                held = jnp.where(k < x, step_a * held + step_b, held)
            held = own_a * held + own_b
            enter_row[it] = held
            enter_copy(it).start()
            twin_a, twin_b = halves(z_maps[it, z * nc])
            here[...] = twin_a * held + twin_b

        return seg[0] * rows_to_lanes(here[...]) + seg[1]

    def apply(p, enter):
        at = pl.ds(p * group, group)
        hist[pl.ds(1 + p * group, group)] = pre_a[at] * enter + pre_b[at]

    send_block(0, ORDERS[0][0])
    table_copy.start()
    weight_copy.start()
    for copy in rows_copies:
        copy.wait()
    edge_copy.wait()
    first = lax.broadcasted_iota(jnp.int32, (SEGS, width), 0) == 0
    outer = jnp.where(tm == 0, jnp.broadcast_to(init_ref[...], (SEGS, width)), pltpu.roll(edge[...], 1, 0))
    hist[0] = jnp.where(first, outer, pltpu.roll(hist[steps], 1, 0))
    for p in ORDERS[0][1:]:
        send_block(0, p)

    table_copy.wait()

    def split(g, _):
        rest = table[g]
        for k in range(3):
            part = rest.astype(BF16)
            pieces[k, g] = part
            rest = rest - part.astype(F32)

    lax.fori_loop(0, 3, split, None)
    lane = lax.broadcasted_iota(jnp.int32, (SEGS, vocab), 1)
    lines = []
    for s in range(SEGS):
        tile = s * steps // LANES * LANES
        line = ids_ref[:, tile : tile + LANES]
        back = s * steps - tile
        lines.append(pltpu.roll(line, LANES - back, 1) if back else line)
    by_segment = jnp.concatenate(lines, 0)

    def mark(k, _):
        ids = pltpu.roll(by_segment, lax.rem(LANES - k * 8, LANES), 1)
        for u in range(0, 8, 2):
            both = [jnp.where(ids[:, v : v + 1] == lane, 1.0, 0.0) for v in (u, u + 1)]
            at = pl.ds(pl.multiple_of((k * 8 + u) * SEGS, 2 * SEGS), 2 * SEGS)
            onehot[at] = jnp.concatenate(both, 0).astype(BF16)

    lax.fori_loop(0, steps // 8, mark, None)

    def look_up(p, _):
        for g in range(3):
            found = dot(onehot[block_rows(p)], pieces[0, g])
            found += dot(onehot[block_rows(p)], pieces[1, g])
            found += dot(onehot[block_rows(p)], pieces[2, g])
            if g == 0:
                found += zb_ref[...]
            inp[g, block_rows(p)] = found

    lax.fori_loop(0, BLOCKS, look_up, None)

    weight_copy.wait()
    same = lax.broadcasted_iota(jnp.int32, (LANES, LANES), 0) == lax.broadcasted_iota(
        jnp.int32, (LANES, LANES), 1
    )
    for g in range(3):
        for k in range(tiles):
            at = pl.ds(pl.multiple_of(y * width + k * LANES, LANES), LANES)
            corner = weight[g, at, k * LANES : (k + 1) * LANES].astype(F32)
            line = jnp.sum(jnp.where(same, corner, 0.0), 0, keepdims=True)
            diag[g, :, k * LANES : (k + 1) * LANES] = jnp.broadcast_to(line, (SEGS, LANES))

    run_a, run_b, first_err = sweep(0)
    enter = entering(0, run_a, run_b, None)
    hist[0] = enter
    enters[y] = enter
    for k in range(3):
        lead_enter(k, y).start()
    for p in ORDERS[1]:
        apply(p, enter)
        send_block(1, p)
    first_sum = sum_tiles(first_err)

    run_a, run_b, second_err = sweep(1)
    second_sum = sum_tiles(second_err)
    enter = entering(1, run_a, run_b, (first_sum, second_sum))

    for p in range(BLOCKS):
        apply(p, enter)

    @pl.when(c == 1)
    def _():
        wait_bytes(plane_res.at[pl.ds(0, plane - 1)], res_sem.at[2, 1])
        sum_row[...] = functools.reduce(jnp.add, [plane_res[k] for k in range(plane)])
        sum_copy().start()
        for it in range(ITERS):
            wait_bytes(z_maps.at[it, pl.ds(0, nz - 1)], z_sem.at[it, 0])
            wait_bytes(x_maps.at[it, pl.ds(0, nx - 1)], x_sem.at[it, 0])
            enter_copy(it).wait_send()
        wait_bytes(z_res.at[pl.ds(0, nz - 1)], res_sem.at[1, 0])
        wait_bytes(plane_res.at[pl.ds(0, plane - 1)], res_sem.at[2, 0])
        sum_copy().wait_send()

    @pl.when(c == 0)
    def _():
        for it in range(ITERS):
            wait_bytes(z_maps.at[it, pl.ds(0, nz)], z_sem.at[it, 0])
        wait_bytes(z_res.at[pl.ds(0, nz)], res_sem.at[1, 0])
        sum_copy().wait_recv()

    sums_ref[...] = sum_row[...]
    wait_bytes(enters.at[pl.ds(0, 3)], lead_sem.at[1])
    for it in range(ITERS):
        skip = lead if it else 0
        wait_bytes(sent.at[it, pl.ds(0, 3), pl.ds(skip, rows - skip)], send_sem.at[it])


def write_out(count, hist, sums_ref, out_hbm, res_ref, out_sem):
    steps = hist.shape[0] - 1
    copies = [
        pltpu.make_async_copy(
            hist.at[pl.ds(1, steps), s], out_hbm.at[pl.ds(s * steps, steps)], out_sem.at[s]
        )
        for s in range(SEGS)
    ]
    for copy in copies:
        copy.start()
    norms = jnp.sqrt(jnp.sum(sums_ref[...], 1, keepdims=True) / count)
    for it in range(ITERS):
        res_ref[it] = norms[it, 0]
    for copy in copies:
        copy.wait()


def sum_tiles(err):
    return functools.reduce(
        jnp.add, [err[:, k : k + LANES] for k in range(0, err.shape[1], LANES)]
    )


def per_device(token_ids, input_table, recur_weight, z_bias, hn_bias, init_state, guess):
    rows, width = guess.shape
    vocab, full = input_table.shape[0], recur_weight.shape[0]
    nx, nz, nc, ny = (lax.axis_size(a) for a in (*TM, "hid"))
    steps, plane, tiles = rows // SEGS, nx * ny, width // LANES
    anywhere = pl.BlockSpec(memory_space=pl.ANY)
    vmem = pl.BlockSpec(memory_space=pltpu.VMEM)
    sem = pltpu.SemaphoreType.DMA
    hist, sums = pl.pallas_call(
        functools.partial(kernel, (nx, nz, nc, ny, rows, width, vocab)),
        out_shape=(
            pltpu.VMEM((steps + 1, SEGS, width), F32),
            pltpu.VMEM((ITERS, LANES), F32),
        ),
        in_specs=[pl.BlockSpec(memory_space=pltpu.HBM)] * 7,
        out_specs=(vmem, vmem),
        scratch_shapes=[
            pltpu.VMEM((1, rows), jnp.int32),
            pltpu.VMEM((1, width), F32),
            pltpu.VMEM((1, width), F32),
            pltpu.VMEM((1, width), F32),
            pltpu.VMEM((3, vocab, width), F32),
            pltpu.VMEM((3, 3, vocab, width), BF16),
            pltpu.VMEM((3, full, width), BF16),
            pltpu.VMEM((ITERS, ny, rows, width), BF16),
            pltpu.VMEM((rows, vocab), BF16),
            pltpu.VMEM((3, rows, width), F32),
            pltpu.VMEM((3, rows, width), F32),
            pltpu.VMEM((steps, SEGS, width), F32),
            pltpu.VMEM((steps, SEGS, width), F32),
            pltpu.VMEM((3, SEGS, width), F32),
            pltpu.VMEM((2, SEGS, width), F32),
            pltpu.VMEM((SEGS, width), F32),
            pltpu.VMEM((ITERS, nz * nc, 2 * tiles, LANES), F32),
            pltpu.VMEM((ITERS, nx, 2 * tiles, LANES), F32),
            pltpu.VMEM((ITERS, tiles, LANES), F32),
            pltpu.VMEM((tiles, LANES), F32),
            pltpu.VMEM((nz * nc, ITERS, LANES), F32),
            pltpu.VMEM((plane, ITERS, LANES), F32),
            pltpu.VMEM((ITERS, LANES), F32),
            pltpu.VMEM((ny, 2, steps // 16 - 1, SEGS, width), F32),
            pltpu.VMEM((ny, SEGS, width), F32),
            sem((SEGS + 4,)),
            sem((2,)),
            sem((2,)),
            sem((ITERS,)),
            sem((ITERS, 2, BLOCKS)),
            sem((ITERS, 2, BLOCKS)),
            sem((ITERS, 2)),
            sem((ITERS, 2)),
            sem((ITERS, 2)),
            sem((4, 2)),
            sem((11,)),
        ],
        compiler_params=pltpu.CompilerParams(
            collective_id=0, has_side_effects=True, vmem_limit_bytes=40 * 1024 * 1024
        ),
    )(
        *(
            pltpu.with_memory_space_constraint(array, pltpu.HBM)
            for array in (
                token_ids[None],
                jnp.transpose(input_table, (1, 0, 2)),
                jnp.transpose(recur_weight, (1, 0, 2)),
                z_bias[None],
                hn_bias[None],
                init_state[None],
                guess,
            )
        )
    )
    return pl.pallas_call(
        functools.partial(write_out, nx * nz * nc * rows * ny * width),
        out_shape=(
            jax.ShapeDtypeStruct((rows, width), F32),
            jax.ShapeDtypeStruct((ITERS,), F32),
        ),
        in_specs=[vmem, vmem],
        out_specs=(anywhere, pl.BlockSpec(memory_space=pltpu.SMEM)),
        scratch_shapes=[sem((SEGS,))],
        compiler_params=pltpu.CompilerParams(vmem_limit_bytes=8 * 1024 * 1024),
    )(hist, sums)


def solution(mesh):
    chips = mesh.devices.shape[0]
    nz, nc = (8, 2) if chips == 64 else (2, 2)
    finer = Mesh(
        mesh.devices.reshape(chips // (nz * nc), nz, nc, mesh.shape["hid"]), (*TM, "hid")
    )
    in_specs = (
        P(TM),
        P(None, None, "hid"),
        P(None, None, "hid"),
        P("hid"),
        P("hid"),
        P("hid"),
        P(TM, "hid"),
    )
    return jax.shard_map(
        per_device, mesh=finer, in_specs=in_specs, out_specs=(P(TM, "hid"), P()), check_vma=False
    )
```
